256 devices in a mesh: mission: 8 (over x, z_lo), arc: 32 (over z_hi, y, core).
Axes of the slice: x: 4, y: 4, z: 8 (z_hi: 4, z_lo: 2; z = z_hi * 2 + z_lo), core: 2. Of those that a mesh axis runs over, the one named last changes fastest.
Arguments:
- design: bfloat16 [20480, 5120], P(('mission', 'arc')), may hold values from -3 to 3
- nuisance_design: bfloat16 [20480, 128], P(('mission', 'arc')), may hold values from -1 to 1
- observed: float32 [20480], P(('mission', 'arc')), may hold values from -6 to 6
- arc_of_row: int32 [20480], P(('mission', 'arc')), may hold values from 0 to 1, as said below
- nuis_size: int32 [512], P(('mission', 'arc')), may hold values from 32 to 128
- weight_index: int32 [20480], P(('mission', 'arc')), may hold values from 0 to 7
- kind_weight: float32 [8], replicated, may hold values from 0.3 to 3
- mission_weight: float32 [8], P('mission'), may hold values from 0.3 to 3
Outputs:
- normal_fold: float32 [2560, 5120], P(('mission', 'arc'))
- right_side: float32 [5120], P(('mission', 'arc'))
- tail_diagonal: float32 [2560], P(('mission', 'arc'))
The draws below stay inside these ranges and needn't reach their ends.
Inputs may be any that keep to these rules, and one draw needn't show every extreme that they name: `arc_of_row`: in each row block of 80 rows the rows of arc 0 come first and those of arc 1 follow; each arc has at least 20 rows.
All inputs are finite; a program needn't handle non-finite values.
Results may differ from the reference program's by a relative error of at most 0.019.
Values may be sent and summed in bfloat16 or wider, within the bound.
A program may use at most 192 MiB of HBM per device.

```python
import math
import jax
import jax.numpy as jnp
from jax import lax

P_SIZE = 5120
NUIS = 128
KINDS = 8
ARCS_DEV = 2
OBS_DEV = 80
HALF = 2560
OBS = 20480
ARCS = 512
N_MISSION = 8
N_ARC = 32


def draw_design(key, part):
    noise_key = jax.random.fold_in(jax.random.fold_in(key, 11), 0)
    freq_key = jax.random.fold_in(jax.random.fold_in(key, 11), 1)
    phase_key = jax.random.fold_in(jax.random.fold_in(key, 11), 2)
    perm_key = jax.random.fold_in(jax.random.fold_in(key, 11), 4)
    columns = jnp.arange(P_SIZE, dtype=jnp.float32)
    noise_part = jnp.clip(jax.random.normal(noise_key, (OBS, P_SIZE), jnp.float32), -6.0, 6.0)
    mode_count = 4
    frequency = jnp.exp(jax.random.uniform(freq_key, (OBS, mode_count), jnp.float32, math.log(0.001), 0.0))
    phases = jax.random.uniform(phase_key, (OBS, mode_count), jnp.float32, -math.pi, math.pi)
    smooth = jnp.zeros((OBS, P_SIZE), jnp.float32)
    for mode_id in range(mode_count):
        smooth = smooth + jnp.cos(frequency[:, mode_id:mode_id + 1] * columns[None, :] + phases[:, mode_id:mode_id + 1])
    values = noise_part + math.sqrt(2.0 / mode_count) * smooth
    blocks = OBS // OBS_DEV
    block_width = P_SIZE // blocks
    target = jax.random.permutation(perm_key, blocks)
    row_block = jnp.arange(OBS, dtype=jnp.int32) // OBS_DEV
    col_block = jnp.arange(P_SIZE, dtype=jnp.int32) // block_width
    spike_gain = jnp.where(target[row_block][:, None] == col_block[None, :], 6.0, 1.0)
    scaled = values * spike_gain / math.sqrt(OBS)
    return jnp.clip(scaled, -3.0, 3.0).astype(jnp.bfloat16)


def draw_arc_of_row(key, part):
    blocks = OBS // OBS_DEV
    split_at = jax.random.randint(jax.random.fold_in(key, 23), (blocks, 1), OBS_DEV // 4, 3 * OBS_DEV // 4 + 1)
    position = jnp.arange(OBS_DEV, dtype=jnp.int32)[None, :]
    return (position >= split_at).astype(jnp.int32).reshape(OBS)


def touch_ends(values, rng, least, top_value):
    shape = values.shape
    index_at = [jax.random.randint(jax.random.fold_in(rng, axis), (), 0, shape[axis]) for axis in range(len(shape))]
    values = values.at[tuple(index_at)].set(least)
    longest = shape.index(max(shape))
    index_at[longest] = (index_at[longest] + 1) % shape[longest]
    return values.at[tuple(index_at)].set(top_value)


def block_levels(key, extent, pieces, least, top_value):
    loudness = 1.0
    for axis_at, parts in pieces:
        steps = jax.random.uniform(jax.random.fold_in(jax.random.fold_in(key, 6), axis_at), (parts,), jnp.float32, least / len(pieces), top_value / len(pieces))
        loudness = loudness * jnp.repeat(jnp.exp(steps), extent[axis_at] // parts).reshape((-1,) + (1,) * (len(extent) - 1 - axis_at))
    return loudness


def normal_values(key, dims, deviation, reach, cuts=(), held_as=jnp.bfloat16):
    level = block_levels(key, dims, cuts, -0.22, 0.18) if cuts else 1.0
    array = jax.random.normal(key, dims, jnp.float32) * deviation * level
    return jnp.minimum(jnp.maximum(array, -reach), reach).astype(held_as)


def setup_inputs(seed: int = 0) -> dict:
    keys = jax.random.split(jax.random.key(seed), 9)
    return {
        "design": draw_design(jax.random.fold_in(keys[8], 71), 0),
        "nuisance_design": normal_values(keys[1], (OBS, NUIS), (OBS_DEV // 2) ** -0.5, 1.0, ((0, 256),)),
        "observed": normal_values(keys[2], (OBS,), 1.0, 6.0, ((0, 256),), jnp.float32),
        "arc_of_row": draw_arc_of_row(jax.random.fold_in(keys[8], 71), 0),
        "nuis_size": touch_ends(jax.random.randint(keys[4], (ARCS,), NUIS // 4, NUIS + 1), jax.random.fold_in(keys[4], 1), NUIS // 4, NUIS).astype(jnp.int32),
        "weight_index": touch_ends(jax.random.randint(keys[5], (OBS,), 0, KINDS), jax.random.fold_in(keys[5], 1), 0, KINDS - 1).astype(jnp.int32),
        "kind_weight": jnp.clip(jnp.exp(jax.random.uniform(keys[6], (KINDS,), jnp.float32, math.log(0.3), math.log(3.0))), 0.3, 3.0),
        "mission_weight": jnp.clip(jnp.exp(math.log(3.0) - 2.3025851 * jax.random.uniform(keys[7], (N_MISSION,), jnp.float32) ** block_levels(keys[7], (N_MISSION,), ((0, 8),), -0.2, 0.2)), 0.3, 3.0),
    }


def local_system(design, nuisance_design, observed, arc_of_row, nuis_size, weight_index, kind_weight):
    kind_ids = jnp.arange(kind_weight.shape[0], dtype=jnp.int32)
    row_weight = jnp.sum(jnp.where(weight_index[:, None] == kind_ids[None, :], kind_weight[None, :], 0.0), axis=1)
    nuis_ids = jnp.arange(nuisance_design.shape[1], dtype=jnp.int32)
    eye_block = jnp.eye(nuisance_design.shape[1], dtype=jnp.float32)
    blocks = []
    solved = []
    solved_obs = []
    for arc_id in range(ARCS_DEV):
        col_mask = (nuis_ids < nuis_size[arc_id]).astype(jnp.bfloat16)
        in_arc = (arc_of_row == arc_id).astype(jnp.float32)
        masked = nuisance_design * col_mask[None, :]
        weighted = (masked.astype(jnp.float32) * (row_weight * in_arc)[:, None]).astype(jnp.bfloat16)
        normal_ll = jnp.dot(weighted.T.astype(jnp.float32), masked.astype(jnp.float32), preferred_element_type=jnp.float32) + eye_block
        coupling = jnp.dot(weighted.T.astype(jnp.float32), design.astype(jnp.float32), preferred_element_type=jnp.float32)
        obs_part = jnp.dot(weighted.T.astype(jnp.float32), observed, precision=lax.Precision.HIGHEST)
        factor = jnp.linalg.cholesky(normal_ll)
        blocks.append(weighted)
        solved.append(jax.scipy.linalg.cho_solve((factor, True), coupling).astype(jnp.bfloat16))
        solved_obs.append(jax.scipy.linalg.cho_solve((factor, True), obs_part))
    stacked = jnp.concatenate(blocks, axis=1)
    solved_all = jnp.concatenate(solved, axis=0)
    obs_all = jnp.concatenate(solved_obs, axis=0)
    reduced = (row_weight[:, None] * design.astype(jnp.float32) - jnp.dot(stacked.astype(jnp.float32), solved_all.astype(jnp.float32), preferred_element_type=jnp.float32)).astype(jnp.bfloat16)
    reduced_obs = (row_weight * observed - jnp.dot(stacked.astype(jnp.float32), obs_all, precision=lax.Precision.HIGHEST)).astype(jnp.bfloat16)
    right_term = jnp.dot(reduced_obs.astype(jnp.float32), design.astype(jnp.float32), preferred_element_type=jnp.float32)
    half_width = design.shape[1] // 2
    tail_term = jnp.sum(design[:, half_width:].astype(jnp.float32) * reduced[:, half_width:].astype(jnp.float32), axis=0)
    return (reduced, right_term, tail_term)

def reference(design, nuisance_design, observed, arc_of_row, nuis_size, weight_index, kind_weight, mission_weight):
    devices = N_MISSION * N_ARC
    col_ids = jnp.arange(P_SIZE, dtype=jnp.int32)
    row_ids = jnp.arange(HALF, dtype=jnp.int32)
    keep_upper = col_ids[None, :] >= row_ids[:, None]

    def per_block(totals, block_id):
        fold_total, right_total, tail_total = totals
        row_start = (block_id * OBS_DEV).astype(jnp.int32)
        arc_start = (block_id * ARCS_DEV).astype(jnp.int32)
        block_design = lax.dynamic_slice_in_dim(design, row_start, OBS_DEV, 0)
        block_nuis = lax.dynamic_slice_in_dim(nuisance_design, row_start, OBS_DEV, 0)
        block_obs = lax.dynamic_slice_in_dim(observed, row_start, OBS_DEV, 0)
        block_arcs = lax.dynamic_slice_in_dim(arc_of_row, row_start, OBS_DEV, 0)
        block_kinds = lax.dynamic_slice_in_dim(weight_index, row_start, OBS_DEV, 0)
        block_sizes = lax.dynamic_slice_in_dim(nuis_size, arc_start, ARCS_DEV, 0)
        weight = mission_weight[block_id // N_ARC]
        reduced, right_term, tail_term = local_system(block_design, block_nuis, block_obs, block_arcs, block_sizes, block_kinds, kind_weight)
        term_full = weight * jnp.dot(block_design.T.astype(jnp.float32), reduced.astype(jnp.float32), preferred_element_type=jnp.float32)
        folded = jnp.where(keep_upper, term_full[:HALF], term_full[::-1, ::-1][:HALF])
        rounded = lax.optimization_barrier(folded.astype(jnp.bfloat16))
        fold_total = fold_total + rounded.astype(jnp.float32)
        return ((fold_total, right_total + weight * right_term, tail_total + weight * tail_term), None)
    initial = (jnp.zeros((HALF, P_SIZE), jnp.float32), jnp.zeros((P_SIZE,), jnp.float32), jnp.zeros((HALF,), jnp.float32))
    totals, unused_out = lax.scan(per_block, initial, jnp.arange(devices, dtype=jnp.int32))
    return (totals[0], totals[1], totals[2])
```

```python
import jax
import jax.numpy as jnp
from jax import lax
from jax.experimental import pallas as pl
from jax.experimental.pallas import tpu as pltpu
from jax.sharding import PartitionSpec as P

NX = 4
NY = 4
NZ = 8
OBS = 80
WIDTH = 5120
CHUNK = 640
NCHUNK = 8
ROWS = 320
UNIT = 416
ZUNIT = 112
F32 = jnp.float32
BF16 = jnp.bfloat16
MESH = pl.DeviceIdType.MESH


def split(v):
    hi = v.astype(BF16)
    lo = (v - hi.astype(F32)).astype(BF16)
    return hi, lo


def iota(shape, dim):
    return lax.broadcasted_iota(jnp.int32, shape, dim)


def dot(a, b):
    return jnp.dot(a, b, preferred_element_type=F32)


def dot_t(a, b):
    return lax.dot_general(a, b, (((1,), (1,)), ((), ())), preferred_element_type=F32)


def kernel(
    ns_ref,
    kw_ref,
    mw_ref,
    design_ref,
    nuis_ref,
    obs_ref,
    arc_ref,
    kind_ref,
    out_ref,
    small_ref,
    dall,
    aall,
    vsend,
    vall,
    ahi,
    alo,
    tt,
    bout,
    rrel,
    rdir,
    rsum,
    fz,
    zf,
    zs,
    zr,
    of,
    ld_sem,
    xs_p,
    xs_m,
    xf_p,
    xf_m,
    xr,
    ps,
    pr,
    as_sem,
    ar,
    aps,
    apr,
    vs_sem,
    vr,
    ys1,
    ys2,
    ys3,
    yr1,
    yr2,
    yr3,
    zs_sem,
    zr_sem,
):
    mission = lax.axis_index("mission")
    arc = lax.axis_index("arc")
    x = mission // 2
    zl = mission % 2
    zh = arc // 8
    y = (arc // 2) % 4
    core = arc % 2
    s = 4 * zl + zh
    other = 1 - core

    def dev(dx, dy, ds, dc):
        return (2 * dx + ds // 4, 8 * (ds % 4) + 2 * dy + dc)

    xp = (x + 1) % 4
    xm = (x + 3) % 4
    x2 = (x + 2) % 4
    yp = (y + 1) % 4
    ym = (y + 3) % 4

    def block(b):
        return pl.ds(pl.multiple_of(b * OBS, OBS), OBS)

    def load(c):
        return pltpu.make_async_copy(
            design_ref.at[:, pl.ds(c * CHUNK, CHUNK)],
            dall.at[c, block(core), :],
            ld_sem.at[c],
        )

    for c in range(NCHUNK):
        load(c).start()

    barrier = pltpu.get_barrier_semaphore()
    peers = [dev(xp, y, s, core), dev(xm, y, s, core), dev(x2, y, s, core)]
    peers += [dev(xp, y, s, other), dev(xm, y, s, other), dev(x2, y, s, other)]
    peers += [dev(x, y, s, other), dev(x, yp, s, core), dev(x, ym, s, core)]
    for d in range(1, NZ):
        peers.append(dev(x, y, (s + d) % NZ, core))
    for peer in peers:
        pl.semaphore_signal(barrier, inc=1, device_id=peer, device_id_type=MESH)
    pl.semaphore_wait(barrier, len(peers))

    def remote(src, dst, ssem, rsem, to):
        return pltpu.make_async_remote_copy(
            src_ref=src, dst_ref=dst, send_sem=ssem, recv_sem=rsem, device_id=to, device_id_type=MESH
        )

    def own_p(c):
        return remote(
            dall.at[c, block(core), :],
            dall.at[c, block(2 + core), :],
            xs_p.at[c],
            xr.at[0, c],
            dev(xp, y, s, core),
        )

    def own_m(c):
        return remote(
            dall.at[c, block(core), :],
            dall.at[c, block(4 + core), :],
            xs_m.at[c],
            xr.at[1, c],
            dev(xm, y, s, core),
        )

    def fwd_p(p):
        return remote(
            dall.at[p, block(2 + core), :],
            dall.at[p, block(6 + core), :],
            xf_p.at[p],
            xr.at[2, p],
            dev(xp, y, s, core),
        )

    def fwd_m(p):
        c = 7 - p
        return remote(
            dall.at[c, block(4 + core), :],
            dall.at[c, block(6 + core), :],
            xf_m.at[p],
            xr.at[2, c],
            dev(xm, y, s, core),
        )

    def recv_x(slot, c):
        ref = dall.at[c, block(2 * slot + core), :]
        return remote(ref, ref, xs_p.at[c], xr.at[slot - 1, c], dev(xp, y, s, core))

    def partner(slot, c):
        ref = dall.at[c, block(2 * slot + core), :]
        return remote(ref, ref, ps.at[slot, c], pr.at[slot, c], dev(x, y, s, other))

    def recv_partner(slot, c):
        ref = dall.at[c, block(2 * slot + other), :]
        return remote(ref, ref, ps.at[slot, c], pr.at[slot, c], dev(x, y, s, other))

    def pair(e, mine):
        if e == 0:
            return mine
        return (e - 1) + (e - 1 >= mine).astype(jnp.int32)

    for c in range(NCHUNK):
        load(c).wait()

    own_p(xp).start()
    own_m(7 - xm).start()
    own_p(7 - xp).start()
    own_m(xm).start()
    own_p(x2).start()
    own_m(7 - x2).start()

    for e in range(4):
        p = pair(e, x)
        partner(0, p).start()
        partner(0, 7 - p).start()

    def own_rest(e):
        pp = pair(e, xp)
        pm = pair(e, xm)

        @pl.when(pp != x2)
        def _():
            own_p(pp).start()

        own_m(pm).start()
        own_p(7 - pp).start()

        @pl.when(pm != x2)
        def _():
            own_m(7 - pm).start()

    own_rest(1)

    lane = iota((OBS, 128), 1)
    sub = iota((OBS, 128), 0)
    eye = lane == sub
    arc_row = jnp.concatenate([arc_ref[...], jnp.full((1, 48), 2, jnp.int32)], axis=1).astype(F32)
    kind_row = jnp.concatenate([kind_ref[...], jnp.zeros((1, 48), jnp.int32)], axis=1)
    obs_row = jnp.concatenate([obs_ref[...], jnp.zeros((1, 48), F32)], axis=1)
    w_row = jnp.zeros((1, 128), F32)
    for k in range(8):
        w_row = jnp.where(kind_row == k, kw_ref[k], w_row)

    def to_col(row):
        return jnp.sum(jnp.where(eye, jnp.broadcast_to(row, (OBS, 128)), 0.0), axis=1, keepdims=True)

    arc_col = to_col(arc_row)
    obs_col = to_col(obs_row)
    size_col = jnp.where(arc_col == 0.0, ns_ref[0], ns_ref[1])
    nuis = jnp.where(lane < size_col, nuis_ref[...].astype(F32), 0.0)
    nuis = jnp.concatenate([nuis, jnp.zeros((48, 128), F32)], axis=0).astype(BF16)
    gram = dot_t(nuis, nuis)[:OBS]
    h = jnp.where(arc_col == arc_row, gram, 0.0) + jnp.where(eye, 1.0 / w_row, 0.0)

    def eliminate(k, h):
        on_col = lane == k
        col = jnp.sum(jnp.where(on_col, h, 0.0), axis=1, keepdims=True)
        row = jnp.sum(jnp.where(sub == k, h, 0.0), axis=0, keepdims=True)
        at = lane[:1] == k
        pivot = jnp.sum(jnp.where(at, row, 0.0), axis=1, keepdims=True)
        row = jnp.where(at, 1.0, row) * (1.0 / pivot)
        return jnp.where(sub == k, row, jnp.where(on_col, 0.0, h) - col * row)

    a = lax.fori_loop(0, OBS, eliminate, h) * mw_ref[0]
    own_b = pl.ds(pl.multiple_of(core * OBS, OBS), OBS)
    aall[own_b, :] = a

    def send_a(slot, to, src_slot, k):
        return remote(
            aall.at[block(2 * src_slot + core), :],
            aall.at[block(2 * slot + core), :],
            as_sem.at[k],
            ar.at[slot - 1],
            to,
        )

    send_a(1, dev(xp, y, s, core), 0, 0).start()
    send_a(2, dev(xm, y, s, core), 0, 1).start()

    def partner_a(slot):
        ref = aall.at[block(2 * slot + core), :]
        return remote(ref, ref, aps.at[slot], apr.at[slot], dev(x, y, s, other))

    def recv_partner_a(slot):
        ref = aall.at[block(2 * slot + other), :]
        return remote(ref, ref, aps.at[slot], apr.at[slot], dev(x, y, s, other))

    partner_a(0).start()

    recv_x(1, xp).wait_recv()
    fwd_p(xp).start()
    recv_x(2, 7 - xm).wait_recv()
    fwd_m(xm).start()
    own_rest(2)
    own_rest(3)
    send_a(1, dev(xp, y, s, core), 0, 0).wait_recv()
    send_a(3, dev(xp, y, s, core), 1, 2).start()
    partner_a(1).start()
    send_a(2, dev(xm, y, s, core), 0, 1).wait_recv()
    partner_a(2).start()

    z_row = jnp.sum(a * obs_col, axis=0, keepdims=True)
    z_hi, z_lo = split(z_row)
    z_two = jnp.concatenate([z_hi.astype(F32), z_lo.astype(F32), jnp.zeros((14, 128), F32)], axis=0)
    z_two = z_two[:, :OBS].astype(BF16)
    a_hi, a_lo = split(a[:, :OBS])
    for c in range(NCHUNK):
        mine = dall[c, own_b, :]
        res = dot(z_two, mine)
        res = res[0:1] + res[1:2]
        for t in range(5):
            tile = 5 * c + t
            vsend[tile // 10, pl.ds(tile % 10, 1), :] = res[:, 128 * t : 128 * t + 128]
        if c >= 4:
            red = dot(a_hi, mine) + dot(a_lo, mine)
            tail = jnp.sum(mine.astype(F32) * red, axis=0, keepdims=True)
            for t in range(5):
                vsend[c - 4, pl.ds(10 + t, 1), :] = tail[:, 128 * t : 128 * t + 128]
    for k in range(4):
        vsend[k, pl.ds(15, 1), :] = jnp.zeros((1, 128), F32)

    v_to = [(x, other), (xp, core), (xp, other), (xm, core), (xm, other), (x2, core), (x2, other)]

    def send_v(k):
        dx, dc = v_to[k]
        return remote(vsend.at[dx], vall.at[k], vs_sem.at[k], vr.at[k], dev(dx, y, s, dc))

    for k in range(7):
        send_v(k).start()

    for slot in (1, 2, 3):
        for c in (x, 7 - x):
            recv_x(slot, c).wait_recv()
            partner(slot, c).start()
    send_a(3, dev(xp, y, s, core), 1, 2).wait_recv()
    partner_a(3).start()
    for k in range(4):
        recv_partner_a(k).wait_recv()

    for b in range(8):
        sel = (iota((128, CHUNK), 1) - OBS * b == iota((128, CHUNK), 0)).astype(F32).astype(BF16)
        hi, lo = split(aall[b * OBS : (b + 1) * OBS, :])
        ahi[b * OBS : (b + 1) * OBS, :] = dot(hi, sel).astype(BF16)
        alo[b * OBS : (b + 1) * OBS, :] = dot(lo, sel).astype(BF16)

    prow = iota((ROWS, CHUNK), 0)
    pcol = iota((ROWS, CHUNK), 1)
    pj = prow >> 3
    py = (pj >= 10).astype(jnp.int32) + (pj >= 20).astype(jnp.int32) + (pj >= 30).astype(jnp.int32)
    target = 80 * (prow & 7) + 20 * py + 10 * core + (pj - 10 * py)

    for slot in range(4):
        recv_partner(slot, x).wait_recv()
        recv_partner(slot, 7 - x).wait_recv()

    for half in range(2):
        hit = (pcol == target) if half == 0 else ((CHUNK - 1 - pcol) == target)
        pick = jnp.where(hit, 1.0, 0.0).astype(BF16)
        chosen = dot_t(pick, dall[x if half == 0 else 7 - x]).astype(BF16)
        tt[half] = (dot(chosen, ahi[...]) + dot(chosen, alo[...])).astype(BF16)

    for k in range(7):
        send_v(k).wait_recv()
    vsum = vsend[x]
    for k in range(7):
        vsum = vsum + vall[k]
    row32 = iota((32, 128), 0)
    lane32 = iota((32, 128), 1)
    spread = jnp.zeros((32, 128), F32)
    for rho in range(15):
        if rho < 10:
            start = 160 * (row32 & 7) + 40 * (row32 >> 3) + 20 * core
            width, at, off = 20, 128 * rho, 0
        else:
            start = 80 * (row32 & 7) + 20 * (row32 >> 3) + 10 * core
            width, at, off = 10, 128 * (rho - 10), 20
        idx = lane32 + at
        keep = (idx >= start) & (idx < start + width)
        vals = jnp.where(keep, jnp.broadcast_to(vsum[rho : rho + 1], (32, 128)), 0.0)
        src = iota((128, 128), 0) + at
        place = iota((128, 128), 1) - off
        quot = (src * (3277 if width == 20 else 6554)) >> 16
        q = jnp.where(src - width * quot == place, 1.0, 0.0).astype(BF16)
        hi, lo = split(vals)
        spread = spread + dot(hi, q) + dot(lo, q)
    for yy in range(4):
        extra = jnp.concatenate([spread[8 * yy : 8 * yy + 8], jnp.zeros((8, 128), F32)], axis=0)
        bout[x, yy, 400:416, :] = extra.astype(BF16)

    def put(q, val):
        for yy in range(4):
            for t in range(5):
                bout[q, yy, 80 * t : 80 * t + 80, :] = val[
                    80 * yy : 80 * yy + 80, 128 * t : 128 * t + 128
                ].astype(BF16)

    rev = jnp.where(iota((128, 128), 0) + iota((128, 128), 1) == 127, 1.0, 0.0).astype(BF16)

    def mirrored(c):
        whole = dall[c]
        parts = []
        for t in range(5):
            parts.append(dot(whole[:, 128 * (4 - t) : 128 * (4 - t) + 128], rev).astype(BF16))
        return jnp.concatenate(parts, axis=1)

    def outputs(p, e):
        put(7 - p, dot(tt[0], dall[7 - p]))
        if e == 0:
            put(p, jnp.where(pcol >= target, dot(tt[0], dall[p]), dot(tt[1], mirrored(7 - p))))
        else:

            @pl.when(p > x)
            def _():
                put(p, dot(tt[0], dall[p]))

            @pl.when(p < x)
            def _():
                put(p, dot(tt[1], mirrored(7 - p)))

            zero = jnp.zeros((16, 128), BF16)
            for yy in range(4):
                bout[p, yy, 400:416, :] = zero
        for yy in range(4):
            bout[7 - p, yy, 400:416, :] = jnp.zeros((16, 128), BF16)

    def y_way(q, up):
        near, far = (yp, ym) if up else (ym, yp)
        far2 = (y + 2) % 4
        s1 = remote(bout.at[q, far2], rrel.at[q], ys1.at[q], yr1.at[q], dev(x, near, s, core))
        s2 = remote(bout.at[q, far], rdir.at[q], ys2.at[q], yr2.at[q], dev(x, far, s, core))
        s3 = remote(bout.at[q, near], rsum.at[q], ys3.at[q], yr3.at[q], dev(x, near, s, core))
        return near, s1, s2, s3

    def y_send(p):
        for q, up in ((p, True), (7 - p, False)):
            near, s1, s2, s3 = y_way(q, up)
            s1.start()
            s2.start()

    def y_relay(p):
        for q, up in ((p, True), (7 - p, False)):
            near, s1, s2, s3 = y_way(q, up)
            s1.wait_recv()
            bout[q, near] = (bout[q, near].astype(F32) + rrel[q].astype(F32)).astype(BF16)
            s3.start()

    def z_copy(p, d):
        to = (s + d) % NZ
        return remote(zs.at[p, to], zr.at[p, s], zs_sem.at[p, to], zr_sem.at[p, s], dev(x, y, to, core))

    def z_recv(p, d):
        frm = (s + d) % NZ
        return remote(zs.at[p, frm], zr.at[p, frm], zs_sem.at[p, frm], zr_sem.at[p, frm], dev(x, y, frm, core))

    zf[...] = jnp.zeros(zf.shape, F32)

    def y_final(p):
        for half, (q, up) in enumerate(((p, True), (7 - p, False))):
            near, s1, s2, s3 = y_way(q, up)
            s2.wait_recv()
            s3.wait_recv()
            fz[half] = bout[q, y].astype(F32) + rdir[q].astype(F32) + rsum[q].astype(F32)
        for k in range(NZ):
            zf[k, 0:50, :] = fz[0, pl.ds(k, 50, stride=8), :]
            zf[k, 50:100, :] = fz[1, pl.ds(k, 50, stride=8), :]
            zf[k, 100:101, :] = fz[0, 400 + k : 401 + k, :]
            zs[p, k] = zf[k].astype(BF16)
        for d in range(1, NZ):
            z_copy(p, d).start()

    def z_final(p, e):
        total = zs[p, s].astype(F32)
        for d in range(1, NZ):
            z_recv(p, d).wait_recv()
            total = total + zr[p, (s + d) % NZ].astype(F32)
        of[...] = total
        for half, q in enumerate((p, 7 - p)):
            for t in range(5):
                at = pl.ds(pl.multiple_of(q * CHUNK + 128 * t, 128), 128)
                out_ref[:, at] = of[50 * half + 10 * t : 50 * half + 10 * t + 10, :]
        if e == 0:
            small_ref[...] = of[100:101, :]

    def relays(e):
        pp = pair(e, xp)
        pm = pair(e, xm)

        @pl.when(pp != x)
        def _():
            recv_x(1, pp).wait_recv()

        fwd_p(pp).start()

        @pl.when(pm != x)
        def _():
            recv_x(2, 7 - pm).wait_recv()

        fwd_m(pm).start()

    def line(e):
        p = pair(e, x)
        for slot in (1, 2, 3):
            for c, upper in ((p, False), (7 - p, True)):
                if slot == 3 or (slot == 1) == upper:
                    recv_x(slot, c).wait_recv()
                partner(slot, c).start()
        for slot in range(4):
            recv_partner(slot, p).wait_recv()
            recv_partner(slot, 7 - p).wait_recv()

    order = [pair(e, x) for e in range(4)]
    outputs(order[0], 0)
    y_send(order[0])
    for e in range(1, 4):
        relays(e)
    line(1)
    y_relay(order[0])
    outputs(order[1], 1)
    y_send(order[1])
    line(2)
    outputs(order[2], 2)
    y_send(order[2])
    y_relay(order[1])
    y_final(order[0])
    line(3)
    outputs(order[3], 3)
    y_send(order[3])
    y_relay(order[2])
    y_final(order[1])
    y_relay(order[3])
    z_final(order[0], 0)
    y_final(order[2])
    z_final(order[1], 1)
    y_final(order[3])
    z_final(order[2], 2)
    z_final(order[3], 3)

    for c in range(NCHUNK):
        own_p(c).wait_send()
        own_m(c).wait_send()
    for p in range(4):
        fwd_p(p).wait_send()
        fwd_m(p).wait_send()
        partner_a(p).wait_send()
        for c in range(NCHUNK):
            partner(p, c).wait_send()
    send_a(1, dev(xp, y, s, core), 0, 0).wait_send()
    send_a(2, dev(xm, y, s, core), 0, 1).wait_send()
    send_a(3, dev(xp, y, s, core), 1, 2).wait_send()
    for k in range(7):
        send_v(k).wait_send()
    for q in range(NCHUNK):
        near, s1, s2, s3 = y_way(q, q < 4)
        s1.wait_send()
        s2.wait_send()
        s3.wait_send()
    for p in range(4):
        for d in range(1, NZ):
            z_copy(p, d).wait_send()


def on_device(design, nuisance, observed, arc_of_row, nuis_size, kinds, kind_weight, mission_weight):
    vmem = pl.BlockSpec(memory_space=pltpu.VMEM)
    smem = pl.BlockSpec(memory_space=pltpu.SMEM)
    dma = pltpu.SemaphoreType.DMA
    scratch = [
        pltpu.VMEM((NCHUNK, 640, CHUNK), BF16),
        pltpu.VMEM((640, 128), F32),
        pltpu.VMEM((4, 16, 128), F32),
        pltpu.VMEM((7, 16, 128), F32),
        pltpu.VMEM((640, 640), BF16),
        pltpu.VMEM((640, 640), BF16),
        pltpu.VMEM((2, ROWS, 640), BF16),
        pltpu.VMEM((NCHUNK, 4, UNIT, 128), BF16),
        pltpu.VMEM((NCHUNK, UNIT, 128), BF16),
        pltpu.VMEM((NCHUNK, UNIT, 128), BF16),
        pltpu.VMEM((NCHUNK, UNIT, 128), BF16),
        pltpu.VMEM((2, UNIT, 128), F32),
        pltpu.VMEM((NZ, ZUNIT, 128), F32),
        pltpu.VMEM((4, NZ, ZUNIT, 128), BF16),
        pltpu.VMEM((4, NZ, ZUNIT, 128), BF16),
        pltpu.VMEM((ZUNIT, 128), F32),
        dma((8,)),
        dma((8,)),
        dma((8,)),
        dma((4,)),
        dma((4,)),
        dma((3, 8)),
        dma((4, 8)),
        dma((4, 8)),
        dma((3,)),
        dma((3,)),
        dma((4,)),
        dma((4,)),
        dma((7,)),
        dma((7,)),
        dma((8,)),
        dma((8,)),
        dma((8,)),
        dma((8,)),
        dma((8,)),
        dma((8,)),
        dma((4, 8)),
        dma((4, 8)),
    ]
    fold, small = pl.pallas_call(
        kernel,
        out_shape=(
            jax.ShapeDtypeStruct((10, WIDTH), F32),
            jax.ShapeDtypeStruct((1, 128), F32),
        ),
        in_specs=[smem, smem, smem, pl.BlockSpec(memory_space=pl.ANY), vmem, vmem, vmem, vmem],
        out_specs=(vmem, vmem),
        scratch_shapes=scratch,
        compiler_params=pltpu.CompilerParams(
            collective_id=0, has_side_effects=True, vmem_limit_bytes=56 * 1024 * 1024
        ),
    )(
        nuis_size,
        kind_weight,
        mission_weight,
        design,
        nuisance,
        observed[None, :],
        arc_of_row[None, :],
        kinds[None, :],
    )
    return (fold, small[0, :20], small[0, 20:30])


def solution(mesh):
    rows = P(("mission", "arc"))
    wide = P(("mission", "arc"), None)
    return jax.shard_map(
        on_device,
        mesh=mesh,
        in_specs=(wide, wide, rows, rows, rows, rows, P(), P("mission")),
        out_specs=(wide, rows, rows),
        check_vma=False,
    )
```

```python
import jax
import jax.numpy as jnp
from jax import lax
from jax.experimental import pallas as pl
from jax.experimental.pallas import tpu as pltpu
from jax.sharding import PartitionSpec as P

NX = 4
NY = 4
NZ = 8
OBS = 80
WIDTH = 5120
CHUNK = 640
NCHUNK = 8
ROWS = 320
UNIT = 416
ZUNIT = 112
F32 = jnp.float32
BF16 = jnp.bfloat16
MESH = pl.DeviceIdType.MESH


def split(v):
    hi = v.astype(BF16)
    lo = (v - hi.astype(F32)).astype(BF16)
    return hi, lo


def iota(shape, dim):
    return lax.broadcasted_iota(jnp.int32, shape, dim)


def dot(a, b):
    return jnp.dot(a, b, preferred_element_type=F32)


def dot_t(a, b):
    return lax.dot_general(a, b, (((1,), (1,)), ((), ())), preferred_element_type=F32)


def kernel(
    ns_ref,
    kw_ref,
    mw_ref,
    design_ref,
    nuis_in,
    obs_in,
    arc_in,
    kind_in,
    out_ref,
    right_ref,
    tail_ref,
    nuis_ref,
    obs_ref,
    arc_ref,
    kind_ref,
    in_sem,
    dall,
    aall,
    vsend,
    vall,
    ahi,
    alo,
    tt,
    bout,
    rrel,
    rdir,
    rsum,
    fz,
    zf,
    zs,
    zr,
    of,
    ld_sem,
    xs_p,
    xs_m,
    xf_p,
    xf_m,
    xr,
    ps,
    pr,
    as_sem,
    ar,
    aps,
    apr,
    vs_sem,
    vr,
    ys1,
    ys2,
    ys3,
    yr1,
    yr2,
    yr3,
    zs_sem,
    zr_sem,
):
    mission = lax.axis_index("mission")
    arc = lax.axis_index("arc")
    x = mission // 2
    zl = mission % 2
    zh = arc // 8
    y = (arc // 2) % 4
    core = arc % 2
    s = 4 * zl + zh
    other = 1 - core

    def dev(dx, dy, ds, dc):
        return (2 * dx + ds // 4, 8 * (ds % 4) + 2 * dy + dc)

    xp = (x + 1) % 4
    xm = (x + 3) % 4
    x2 = (x + 2) % 4
    yp = (y + 1) % 4
    ym = (y + 3) % 4

    def block(b):
        return pl.ds(pl.multiple_of(b * OBS, OBS), OBS)

    def load(c):
        return pltpu.make_async_copy(
            design_ref.at[:, pl.ds(c * CHUNK, CHUNK)],
            dall.at[c, block(core), :],
            ld_sem.at[c],
        )

    small_loads = [
        pltpu.make_async_copy(src, dst, in_sem.at[k])
        for k, (src, dst) in enumerate(
            ((nuis_in, nuis_ref), (obs_in, obs_ref), (arc_in, arc_ref), (kind_in, kind_ref))
        )
    ]
    for c in range(NCHUNK):
        load(c).start()
    for copy in small_loads:
        copy.start()

    barrier = pltpu.get_barrier_semaphore()
    peers = [dev(xp, y, s, core), dev(xm, y, s, core), dev(x2, y, s, core)]
    peers += [dev(xp, y, s, other), dev(xm, y, s, other), dev(x2, y, s, other)]
    peers += [dev(x, y, s, other), dev(x, yp, s, core), dev(x, ym, s, core)]
    for d in range(1, NZ):
        peers.append(dev(x, y, (s + d) % NZ, core))
    for peer in peers:
        pl.semaphore_signal(barrier, inc=1, device_id=peer, device_id_type=MESH)
    pl.semaphore_wait(barrier, len(peers))

    def remote(src, dst, ssem, rsem, to):
        return pltpu.make_async_remote_copy(
            src_ref=src, dst_ref=dst, send_sem=ssem, recv_sem=rsem, device_id=to, device_id_type=MESH
        )

    def own_p(c):
        return remote(
            dall.at[c, block(core), :],
            dall.at[c, block(2 + core), :],
            xs_p.at[c],
            xr.at[0, c],
            dev(xp, y, s, core),
        )

    def own_m(c):
        return remote(
            dall.at[c, block(core), :],
            dall.at[c, block(4 + core), :],
            xs_m.at[c],
            xr.at[1, c],
            dev(xm, y, s, core),
        )

    def fwd_p(p):
        return remote(
            dall.at[p, block(2 + core), :],
            dall.at[p, block(6 + core), :],
            xf_p.at[p],
            xr.at[2, p],
            dev(xp, y, s, core),
        )

    def fwd_m(p):
        c = 7 - p
        return remote(
            dall.at[c, block(4 + core), :],
            dall.at[c, block(6 + core), :],
            xf_m.at[p],
            xr.at[2, c],
            dev(xm, y, s, core),
        )

    def recv_x(slot, c):
        ref = dall.at[c, block(2 * slot + core), :]
        return remote(ref, ref, xs_p.at[c], xr.at[slot - 1, c], dev(xp, y, s, core))

    def partner(slot, c):
        ref = dall.at[c, block(2 * slot + core), :]
        return remote(ref, ref, ps.at[slot, c], pr.at[slot, c], dev(x, y, s, other))

    def recv_partner(slot, c):
        ref = dall.at[c, block(2 * slot + other), :]
        return remote(ref, ref, ps.at[slot, c], pr.at[slot, c], dev(x, y, s, other))

    def pair(e, mine):
        if e == 0:
            return mine
        return (e - 1) + (e - 1 >= mine).astype(jnp.int32)

    for c in range(NCHUNK):
        load(c).wait()

    own_p(xp).start()
    own_m(7 - xm).start()
    own_p(7 - xp).start()
    own_m(xm).start()
    own_p(x2).start()
    own_m(7 - x2).start()

    for e in range(4):
        p = pair(e, x)
        partner(0, p).start()
        partner(0, 7 - p).start()

    def own_lower(e):
        pp = pair(e, xp)
        pm = pair(e, xm)

        @pl.when(pp != x2)
        def _():
            own_p(pp).start()

        own_m(pm).start()

    def own_upper(e):
        pp = pair(e, xp)
        pm = pair(e, xm)
        own_p(7 - pp).start()

        @pl.when(pm != x2)
        def _():
            own_m(7 - pm).start()

    for copy in small_loads:
        copy.wait()

    lane = iota((OBS, 128), 1)
    sub = iota((OBS, 128), 0)
    eye = lane == sub
    arc_row = jnp.concatenate([arc_ref[...], jnp.full((1, 48), 2, jnp.int32)], axis=1).astype(F32)
    kind_row = jnp.concatenate([kind_ref[...], jnp.zeros((1, 48), jnp.int32)], axis=1)
    obs_row = jnp.concatenate([obs_ref[...], jnp.zeros((1, 48), F32)], axis=1)
    w_row = jnp.zeros((1, 128), F32)
    for k in range(8):
        w_row = jnp.where(kind_row == k, kw_ref[k], w_row)

    def to_col(row):
        return jnp.sum(jnp.where(eye, jnp.broadcast_to(row, (OBS, 128)), 0.0), axis=1, keepdims=True)

    arc_col = to_col(arc_row)
    obs_col = to_col(obs_row)
    size_col = jnp.where(arc_col == 0.0, ns_ref[0], ns_ref[1])
    nuis = jnp.where(lane < size_col, nuis_ref[...].astype(F32), 0.0)
    nuis = jnp.concatenate([nuis, jnp.zeros((48, 128), F32)], axis=0).astype(BF16)
    gram = dot_t(nuis, nuis)[:OBS]
    h = jnp.where(arc_col == arc_row, gram, 0.0) + jnp.where(eye, 1.0 / w_row, 0.0)

    def eliminate(step, h):
        k = 2 * step
        on1 = lane == k
        on2 = lane == k + 1
        at1 = on1[:1]
        at2 = on2[:1]
        is1 = sub == k
        is2 = sub == k + 1
        col1 = jnp.sum(jnp.where(on1, h, 0.0), axis=1, keepdims=True)
        col2 = jnp.sum(jnp.where(on2, h, 0.0), axis=1, keepdims=True)
        row1 = jnp.sum(jnp.where(is1, h, 0.0), axis=0, keepdims=True)
        row2 = jnp.sum(jnp.where(is2, h, 0.0), axis=0, keepdims=True)
        p11 = jnp.sum(jnp.where(at1, row1, 0.0), axis=1, keepdims=True)
        p12 = jnp.sum(jnp.where(at2, row1, 0.0), axis=1, keepdims=True)
        p22 = jnp.sum(jnp.where(at2, row2, 0.0), axis=1, keepdims=True)
        inv = 1.0 / (p11 * p22 - p12 * p12)
        row1 = jnp.where(at1, 1.0, jnp.where(at2, 0.0, row1))
        row2 = jnp.where(at2, 1.0, jnp.where(at1, 0.0, row2))
        new1 = (p22 * inv) * row1 - (p12 * inv) * row2
        new2 = (p11 * inv) * row2 - (p12 * inv) * row1
        rest = jnp.where(on1 | on2, 0.0, h) - col1 * new1 - col2 * new2
        return jnp.where(is1, new1, jnp.where(is2, new2, rest))

    a = lax.fori_loop(0, OBS // 2, eliminate, h) * mw_ref[0]
    own_b = pl.ds(pl.multiple_of(core * OBS, OBS), OBS)
    aall[own_b, :] = a

    def send_a(slot):
        to = {1: xp, 2: xm, 3: x2}[slot]
        return remote(
            aall.at[own_b, :],
            aall.at[block(2 * slot + core), :],
            as_sem.at[slot - 1],
            ar.at[slot - 1],
            dev(to, y, s, core),
        )

    for slot in (1, 2, 3):
        send_a(slot).start()

    def partner_a(slot):
        ref = aall.at[block(2 * slot + core), :]
        return remote(ref, ref, aps.at[slot], apr.at[slot], dev(x, y, s, other))

    def recv_partner_a(slot):
        ref = aall.at[block(2 * slot + other), :]
        return remote(ref, ref, aps.at[slot], apr.at[slot], dev(x, y, s, other))

    partner_a(0).start()

    z_row = jnp.sum(a * obs_col, axis=0, keepdims=True)
    z_hi, z_lo = split(z_row)
    z_two = jnp.concatenate([z_hi.astype(F32), z_lo.astype(F32), jnp.zeros((14, 128), F32)], axis=0)
    z_two = z_two[:, :OBS].astype(BF16)
    a_hi, a_lo = split(a[:, :OBS])
    for c in range(NCHUNK):
        mine = dall[c, own_b, :]
        res = dot(z_two, mine)
        res = res[0:1] + res[1:2]
        for t in range(5):
            tile = 5 * c + t
            vsend[tile // 10, pl.ds(tile % 10, 1), :] = res[:, 128 * t : 128 * t + 128]
        if c >= 4:
            red = dot(a_hi, mine) + dot(a_lo, mine)
            tail = jnp.sum(mine.astype(F32) * red, axis=0, keepdims=True)
            for t in range(5):
                vsend[c - 4, pl.ds(10 + t, 1), :] = tail[:, 128 * t : 128 * t + 128]
    for k in range(4):
        vsend[k, pl.ds(15, 1), :] = jnp.zeros((1, 128), F32)

    v_to = [(x, other), (xp, core), (xp, other), (xm, core), (xm, other), (x2, core), (x2, other)]

    def send_v(k):
        dx, dc = v_to[k]
        return remote(vsend.at[dx], vall.at[k], vs_sem.at[k], vr.at[k], dev(dx, y, s, dc))

    for k in range(7):
        send_v(k).start()

    recv_x(1, xp).wait_recv()
    fwd_p(xp).start()
    recv_x(2, 7 - xm).wait_recv()
    fwd_m(xm).start()
    own_lower(1)
    own_upper(1)
    own_lower(2)
    own_upper(2)
    own_lower(3)

    for slot in (1, 2):
        for c in (x, 7 - x):
            recv_x(slot, c).wait_recv()
            partner(slot, c).start()
    for slot in (1, 2, 3):
        send_a(slot).wait_recv()
        partner_a(slot).start()
    for c in (x, 7 - x):
        recv_x(3, c).wait_recv()
        partner(3, c).start()
    for slot in range(4):
        recv_partner_a(slot).wait_recv()

    for b in range(8):
        sel = (iota((128, CHUNK), 1) - OBS * b == iota((128, CHUNK), 0)).astype(F32).astype(BF16)
        hi, lo = split(aall[b * OBS : (b + 1) * OBS, :])
        ahi[b * OBS : (b + 1) * OBS, :] = dot(hi, sel).astype(BF16)
        alo[b * OBS : (b + 1) * OBS, :] = dot(lo, sel).astype(BF16)

    prow = iota((ROWS, CHUNK), 0)
    pcol = iota((ROWS, CHUNK), 1)
    pj = prow >> 3
    py = (pj >= 10).astype(jnp.int32) + (pj >= 20).astype(jnp.int32) + (pj >= 30).astype(jnp.int32)
    target = 80 * (prow & 7) + 20 * py + 10 * core + (pj - 10 * py)

    for k in range(7):
        send_v(k).wait_recv()
    vsum = vsend[x]
    for k in range(7):
        vsum = vsum + vall[k]
    row32 = iota((32, 128), 0)
    lane32 = iota((32, 128), 1)
    spread = jnp.zeros((32, 128), F32)
    for rho in range(15):
        if rho < 10:
            start = 160 * (row32 & 7) + 40 * (row32 >> 3) + 20 * core
            width, at, off = 20, 128 * rho, 0
        else:
            start = 80 * (row32 & 7) + 20 * (row32 >> 3) + 10 * core
            width, at, off = 10, 128 * (rho - 10), 20
        idx = lane32 + at
        keep = (idx >= start) & (idx < start + width)
        vals = jnp.where(keep, jnp.broadcast_to(vsum[rho : rho + 1], (32, 128)), 0.0)
        src = iota((128, 128), 0) + at
        place = iota((128, 128), 1) - off
        quot = (src * (3277 if width == 20 else 6554)) >> 16
        q = jnp.where(src - width * quot == place, 1.0, 0.0).astype(BF16)
        hi, lo = split(vals)
        spread = spread + dot(hi, q) + dot(lo, q)
    for yy in range(4):
        extra = jnp.concatenate([spread[8 * yy : 8 * yy + 8], jnp.zeros((8, 128), F32)], axis=0)
        bout[x, yy, 400:416, :] = extra.astype(BF16)

    for slot in range(4):
        recv_partner(slot, x).wait_recv()
        recv_partner(slot, 7 - x).wait_recv()

    for half in range(2):
        hit = (pcol == target) if half == 0 else ((CHUNK - 1 - pcol) == target)
        pick = jnp.where(hit, 1.0, 0.0).astype(BF16)
        chosen = dot_t(pick, dall[x if half == 0 else 7 - x]).astype(BF16)
        tt[half] = (dot(chosen, ahi[...]) + dot(chosen, alo[...])).astype(BF16)

    def put(q, val):
        for yy in range(4):
            for t in range(5):
                bout[q, yy, 80 * t : 80 * t + 80, :] = val[
                    80 * yy : 80 * yy + 80, 128 * t : 128 * t + 128
                ].astype(BF16)

    rev = jnp.where(iota((128, 128), 0) + iota((128, 128), 1) == 127, 1.0, 0.0).astype(BF16)

    def mirrored(c):
        whole = dall[c]
        parts = []
        for t in range(5):
            parts.append(dot(whole[:, 128 * (4 - t) : 128 * (4 - t) + 128], rev).astype(BF16))
        return jnp.concatenate(parts, axis=1)

    def y_first(q, up):
        near = yp if up else ym
        far2 = (y + 2) % 4
        return remote(bout.at[q, far2], rrel.at[q], ys1.at[q], yr1.at[q], dev(x, near, s, core))

    def y_back(q, up):
        far = ym if up else yp
        return remote(bout.at[q, far], rdir.at[q], ys2.at[q], yr2.at[q], dev(x, far, s, core))

    def y_sum(q, up):
        near = yp if up else ym
        return remote(bout.at[q, near], rsum.at[q], ys3.at[q], yr3.at[q], dev(x, near, s, core))

    def y_send(q, up):
        y_first(q, up).start()
        y_back(q, up).start()

    def y_relay(p):
        for q, up in ((7 - p, False), (p, True)):
            near = yp if up else ym
            y_first(q, up).wait_recv()
            bout[q, near] = (bout[q, near].astype(F32) + rrel[q].astype(F32)).astype(BF16)
            y_sum(q, up).start()

    zero = jnp.zeros((16, 128), BF16)

    def outputs(p, e):
        for yy in range(4):
            bout[7 - p, yy, 400:416, :] = zero
        put(7 - p, dot(tt[0], dall[7 - p]))
        y_send(7 - p, False)
        if e == 0:
            put(p, jnp.where(pcol >= target, dot(tt[0], dall[p]), dot(tt[1], mirrored(7 - p))))
        else:

            @pl.when(p > x)
            def _():
                put(p, dot(tt[0], dall[p]))

            @pl.when(p < x)
            def _():
                put(p, dot(tt[1], mirrored(7 - p)))

            for yy in range(4):
                bout[p, yy, 400:416, :] = zero
        y_send(p, True)

    def z_copy(p, d):
        to = (s + d) % NZ
        return remote(zs.at[p, to], zr.at[p, s], zs_sem.at[p, to], zr_sem.at[p, s], dev(x, y, to, core))

    def z_recv(p, d):
        frm = (s + d) % NZ
        return remote(zs.at[p, frm], zr.at[p, frm], zs_sem.at[p, frm], zr_sem.at[p, frm], dev(x, y, frm, core))

    zf[...] = jnp.zeros(zf.shape, F32)

    def y_final(p):
        for half, (q, up) in enumerate(((p, True), (7 - p, False))):
            y_back(q, up).wait_recv()
            y_sum(q, up).wait_recv()
            fz[half] = bout[q, y].astype(F32) + rdir[q].astype(F32) + rsum[q].astype(F32)
        for k in range(NZ):
            zf[k, 0:50, :] = fz[0, pl.ds(k, 50, stride=8), :]
            zf[k, 50:100, :] = fz[1, pl.ds(k, 50, stride=8), :]
            zf[k, 100:101, :] = fz[0, 400 + k : 401 + k, :]
            zs[p, k] = zf[k].astype(BF16)
        for d in range(1, NZ):
            z_copy(p, d).start()

    def z_final(p, e):
        total = zs[p, s].astype(F32)
        for d in range(1, NZ):
            z_recv(p, d).wait_recv()
            total = total + zr[p, (s + d) % NZ].astype(F32)
        of[...] = total
        for half, q in enumerate((p, 7 - p)):
            for t in range(5):
                at = pl.ds(pl.multiple_of(q * CHUNK + 128 * t, 128), 128)
                out_ref[:, at] = of[50 * half + 10 * t : 50 * half + 10 * t + 10, :]
        if e == 0:
            right_ref[...] = of[100:101, 0:20]
            tail_ref[...] = of[100:101, 20:30]

    def relays(e):
        pp = pair(e, xp)
        pm = pair(e, xm)
        need_p = pp != x
        need_m = pm != x
        if e > 1:
            need_p = need_p & (pp != pair(1, x))
            need_m = need_m & (pm != pair(1, x))

        @pl.when(need_p)
        def _():
            recv_x(1, pp).wait_recv()

        fwd_p(pp).start()

        @pl.when(need_m)
        def _():
            recv_x(2, 7 - pm).wait_recv()

        fwd_m(pm).start()

    def line(e):
        p = pair(e, x)
        if e == 1:

            @pl.when((p != xp) & (p != pair(1, xp)))
            def _():
                recv_x(1, p).wait_recv()

            @pl.when((p != xm) & (p != pair(1, xm)))
            def _():
                recv_x(2, 7 - p).wait_recv()

        for slot in (1, 2, 3):
            for c, upper in ((p, False), (7 - p, True)):
                if slot == 3 or (slot == 1) == upper:
                    recv_x(slot, c).wait_recv()
                partner(slot, c).start()
        for slot in range(4):
            recv_partner(slot, p).wait_recv()
            recv_partner(slot, 7 - p).wait_recv()

    order = [pair(e, x) for e in range(4)]
    outputs(order[0], 0)
    relays(1)
    own_upper(3)
    line(1)
    outputs(order[1], 1)
    y_relay(order[0])
    relays(2)
    relays(3)
    line(2)
    outputs(order[2], 2)
    y_relay(order[1])
    line(3)
    outputs(order[3], 3)
    y_final(order[0])
    y_relay(order[2])
    y_final(order[1])
    y_relay(order[3])
    z_final(order[0], 0)
    y_final(order[2])
    z_final(order[1], 1)
    y_final(order[3])
    z_final(order[2], 2)
    z_final(order[3], 3)

    for c in range(NCHUNK):
        own_p(c).wait_send()
        own_m(c).wait_send()
    for p in range(4):
        fwd_p(p).wait_send()
        fwd_m(p).wait_send()
        partner_a(p).wait_send()
        for c in range(NCHUNK):
            partner(p, c).wait_send()
    for slot in (1, 2, 3):
        send_a(slot).wait_send()
    for k in range(7):
        send_v(k).wait_send()
    for q in range(NCHUNK):
        y_first(q, q < 4).wait_send()
        y_back(q, q < 4).wait_send()
        y_sum(q, q < 4).wait_send()
    for p in range(4):
        for d in range(1, NZ):
            z_copy(p, d).wait_send()


def on_device(design, nuisance, observed, arc_of_row, nuis_size, kinds, kind_weight, mission_weight):
    vmem = pl.BlockSpec(memory_space=pltpu.VMEM)
    smem = pl.BlockSpec(memory_space=pltpu.SMEM)
    dma = pltpu.SemaphoreType.DMA
    scratch = [
        pltpu.VMEM((OBS, 128), BF16),
        pltpu.VMEM((1, OBS), F32),
        pltpu.VMEM((1, OBS), jnp.int32),
        pltpu.VMEM((1, OBS), jnp.int32),
        dma((4,)),
        pltpu.VMEM((NCHUNK, 640, CHUNK), BF16),
        pltpu.VMEM((640, 128), F32),
        pltpu.VMEM((4, 16, 128), F32),
        pltpu.VMEM((7, 16, 128), F32),
        pltpu.VMEM((640, 640), BF16),
        pltpu.VMEM((640, 640), BF16),
        pltpu.VMEM((2, ROWS, 640), BF16),
        pltpu.VMEM((NCHUNK, 4, UNIT, 128), BF16),
        pltpu.VMEM((NCHUNK, UNIT, 128), BF16),
        pltpu.VMEM((NCHUNK, UNIT, 128), BF16),
        pltpu.VMEM((NCHUNK, UNIT, 128), BF16),
        pltpu.VMEM((2, UNIT, 128), F32),
        pltpu.VMEM((NZ, ZUNIT, 128), F32),
        pltpu.VMEM((4, NZ, ZUNIT, 128), BF16),
        pltpu.VMEM((4, NZ, ZUNIT, 128), BF16),
        pltpu.VMEM((ZUNIT, 128), F32),
        dma((8,)),
        dma((8,)),
        dma((8,)),
        dma((4,)),
        dma((4,)),
        dma((3, 8)),
        dma((4, 8)),
        dma((4, 8)),
        dma((3,)),
        dma((3,)),
        dma((4,)),
        dma((4,)),
        dma((7,)),
        dma((7,)),
        dma((8,)),
        dma((8,)),
        dma((8,)),
        dma((8,)),
        dma((8,)),
        dma((8,)),
        dma((4, 8)),
        dma((4, 8)),
    ]
    fold, right, tail = pl.pallas_call(
        kernel,
        out_shape=(
            jax.ShapeDtypeStruct((10, WIDTH), F32),
            jax.ShapeDtypeStruct((1, 20), F32),
            jax.ShapeDtypeStruct((1, 10), F32),
        ),
        in_specs=[smem] * 3 + [pl.BlockSpec(memory_space=pl.ANY)] * 5,
        out_specs=(vmem, vmem, vmem),
        scratch_shapes=scratch,
        compiler_params=pltpu.CompilerParams(
            collective_id=0, has_side_effects=True, vmem_limit_bytes=56 * 1024 * 1024
        ),
    )(
        nuis_size,
        kind_weight,
        mission_weight,
        design,
        nuisance,
        observed[None, :],
        arc_of_row[None, :],
        kinds[None, :],
    )
    return (fold, right[0], tail[0])


def solution(mesh):
    rows = P(("mission", "arc"))
    wide = P(("mission", "arc"), None)
    return jax.shard_map(
        on_device,
        mesh=mesh,
        in_specs=(wide, wide, rows, rows, rows, rows, P(), P("mission")),
        out_specs=(wide, rows, rows),
        check_vma=False,
    )
```

```python
import jax
import jax.numpy as jnp
from jax import lax
from jax.experimental import pallas as pl
from jax.experimental.pallas import tpu as pltpu
from jax.sharding import PartitionSpec as P

NX = 4
NY = 4
NZ = 8
OBS = 80
WIDTH = 5120
CHUNK = 640
NCHUNK = 8
ROWS = 320
UNIT = 416
BODY = 400
ZUNIT = 112
F32 = jnp.float32
BF16 = jnp.bfloat16
MESH = pl.DeviceIdType.MESH


def split(v):
    hi = v.astype(BF16)
    lo = (v - hi.astype(F32)).astype(BF16)
    return hi, lo


def iota(shape, dim):
    return lax.broadcasted_iota(jnp.int32, shape, dim)


def dot(a, b):
    return jnp.dot(a, b, preferred_element_type=F32)


def dot_t(a, b):
    return lax.dot_general(a, b, (((1,), (1,)), ((), ())), preferred_element_type=F32)


def kernel(
    ns_in,
    kw_in,
    mw_in,
    design_ref,
    nuis_in,
    obs_in,
    arc_in,
    kind_in,
    out_ref,
    right_ref,
    tail_ref,
    nuis_ref,
    obs_ref,
    arc_ref,
    kind_ref,
    ns_ref,
    kw_ref,
    mw_ref,
    in_sem,
    dall,
    aall,
    vsend,
    vall,
    ahi,
    alo,
    picks,
    tt,
    bout,
    rrel,
    rdir,
    rsum,
    fz,
    zf,
    zs,
    zr,
    of,
    ld_sem,
    xs_p,
    xs_m,
    xf_p,
    xf_m,
    xr,
    ps,
    pr,
    as_sem,
    ar,
    aps,
    apr,
    vs_sem,
    vr,
    ys1,
    ys2,
    ys3,
    yr1,
    yr2,
    yr3,
    zs_sem,
    zr_sem,
):
    mission = lax.axis_index("mission")
    arc = lax.axis_index("arc")
    x = mission // 2
    zl = mission % 2
    zh = arc // 8
    y = (arc // 2) % 4
    core = arc % 2
    s = 4 * zl + zh
    other = 1 - core

    def dev(dx, dy, ds, dc):
        return (2 * dx + ds // 4, 8 * (ds % 4) + 2 * dy + dc)

    xp = (x + 1) % 4
    xm = (x + 3) % 4
    x2 = (x + 2) % 4
    yp = (y + 1) % 4
    ym = (y + 3) % 4

    def block(b):
        return pl.ds(pl.multiple_of(b * OBS, OBS), OBS)

    def load(c):
        return pltpu.make_async_copy(
            design_ref.at[:, pl.ds(c * CHUNK, CHUNK)],
            dall.at[c, block(core), :],
            ld_sem.at[c],
        )

    small_loads = [
        pltpu.make_async_copy(src, dst, in_sem.at[k])
        for k, (src, dst) in enumerate(
            (
                (nuis_in, nuis_ref),
                (obs_in, obs_ref),
                (arc_in, arc_ref),
                (kind_in, kind_ref),
                (ns_in, ns_ref),
                (kw_in, kw_ref),
                (mw_in, mw_ref),
            )
        )
    ]
    for c in range(NCHUNK):
        load(c).start()
    for copy in small_loads:
        copy.start()

    barrier = pltpu.get_barrier_semaphore()
    peers = [dev(xp, y, s, core), dev(xm, y, s, core), dev(x2, y, s, core)]
    peers += [dev(xp, y, s, other), dev(xm, y, s, other), dev(x2, y, s, other)]
    peers += [dev(x, y, s, other), dev(x, yp, s, core), dev(x, ym, s, core)]
    for d in range(1, NZ):
        peers.append(dev(x, y, (s + d) % NZ, core))
    for peer in peers:
        pl.semaphore_signal(barrier, inc=1, device_id=peer, device_id_type=MESH)
    pl.semaphore_wait(barrier, len(peers))

    def remote(src, dst, ssem, rsem, to):
        return pltpu.make_async_remote_copy(
            src_ref=src, dst_ref=dst, send_sem=ssem, recv_sem=rsem, device_id=to, device_id_type=MESH
        )

    def own_p(c):
        return remote(
            dall.at[c, block(core), :],
            dall.at[c, block(2 + core), :],
            xs_p.at[c],
            xr.at[0, c],
            dev(xp, y, s, core),
        )

    def own_m(c):
        return remote(
            dall.at[c, block(core), :],
            dall.at[c, block(4 + core), :],
            xs_m.at[c],
            xr.at[1, c],
            dev(xm, y, s, core),
        )

    def fwd_p(p):
        return remote(
            dall.at[p, block(2 + core), :],
            dall.at[p, block(6 + core), :],
            xf_p.at[p],
            xr.at[2, p],
            dev(xp, y, s, core),
        )

    def fwd_m(p):
        c = 7 - p
        return remote(
            dall.at[c, block(4 + core), :],
            dall.at[c, block(6 + core), :],
            xf_m.at[p],
            xr.at[2, c],
            dev(xm, y, s, core),
        )

    def recv_x(slot, c):
        ref = dall.at[c, block(2 * slot + core), :]
        return remote(ref, ref, xs_p.at[c], xr.at[slot - 1, c], dev(xp, y, s, core))

    def partner(slot, c):
        ref = dall.at[c, block(2 * slot + core), :]
        return remote(ref, ref, ps.at[slot, c], pr.at[slot, c], dev(x, y, s, other))

    def recv_partner(slot, c):
        ref = dall.at[c, block(2 * slot + other), :]
        return remote(ref, ref, ps.at[slot, c], pr.at[slot, c], dev(x, y, s, other))

    def pair(e, mine):
        if e == 0:
            return mine
        return (e - 1) + (e - 1 >= mine).astype(jnp.int32)

    for c in range(NCHUNK):
        load(c).wait()

    own_p(xp).start()
    own_m(7 - xm).start()
    own_p(7 - xp).start()
    own_m(xm).start()
    own_p(x2).start()
    own_m(7 - x2).start()

    for e in range(4):
        p = pair(e, x)
        partner(0, p).start()
        partner(0, 7 - p).start()

    def own_lower(e):
        pp = pair(e, xp)
        pm = pair(e, xm)

        @pl.when(pp != x2)
        def _():
            own_p(pp).start()

        own_m(pm).start()

    def own_upper(e):
        pp = pair(e, xp)
        pm = pair(e, xm)
        own_p(7 - pp).start()

        @pl.when(pm != x2)
        def _():
            own_m(7 - pm).start()

    for copy in small_loads:
        copy.wait()

    lane = iota((OBS, 128), 1)
    sub = iota((OBS, 128), 0)
    eye = lane == sub
    arc_row = jnp.concatenate([arc_ref[...], jnp.full((1, 48), 2, jnp.int32)], axis=1).astype(F32)
    kind_row = jnp.concatenate([kind_ref[...], jnp.zeros((1, 48), jnp.int32)], axis=1)
    obs_row = jnp.concatenate([obs_ref[...], jnp.zeros((1, 48), F32)], axis=1)
    w_row = jnp.zeros((1, 128), F32)
    for k in range(8):
        w_row = jnp.where(kind_row == k, kw_ref[k], w_row)

    def to_col(row):
        return jnp.sum(jnp.where(eye, jnp.broadcast_to(row, (OBS, 128)), 0.0), axis=1, keepdims=True)

    arc_col = to_col(arc_row)
    obs_col = to_col(obs_row)
    size_col = jnp.where(arc_col == 0.0, ns_ref[0], ns_ref[1])
    nuis = jnp.where(lane < size_col, nuis_ref[...].astype(F32), 0.0)
    nuis = jnp.concatenate([nuis, jnp.zeros((48, 128), F32)], axis=0).astype(BF16)
    gram = dot_t(nuis, nuis)[:OBS]
    h = jnp.where(arc_col == arc_row, gram, 0.0) + jnp.where(eye, 1.0 / w_row, 0.0)

    def eliminate(step, h):
        k = 2 * step
        on1 = lane == k
        on2 = lane == k + 1
        at1 = on1[:1]
        at2 = on2[:1]
        is1 = sub == k
        is2 = sub == k + 1
        col1 = jnp.sum(jnp.where(on1, h, 0.0), axis=1, keepdims=True)
        col2 = jnp.sum(jnp.where(on2, h, 0.0), axis=1, keepdims=True)
        row1 = jnp.sum(jnp.where(is1, h, 0.0), axis=0, keepdims=True)
        row2 = jnp.sum(jnp.where(is2, h, 0.0), axis=0, keepdims=True)
        p11 = jnp.sum(jnp.where(at1, row1, 0.0), axis=1, keepdims=True)
        p12 = jnp.sum(jnp.where(at2, row1, 0.0), axis=1, keepdims=True)
        p22 = jnp.sum(jnp.where(at2, row2, 0.0), axis=1, keepdims=True)
        inv = 1.0 / (p11 * p22 - p12 * p12)
        row1 = jnp.where(at1, 1.0, jnp.where(at2, 0.0, row1))
        row2 = jnp.where(at2, 1.0, jnp.where(at1, 0.0, row2))
        new1 = (p22 * inv) * row1 - (p12 * inv) * row2
        new2 = (p11 * inv) * row2 - (p12 * inv) * row1
        rest = jnp.where(on1 | on2, 0.0, h) - col1 * new1 - col2 * new2
        return jnp.where(is1, new1, jnp.where(is2, new2, rest))

    a = lax.fori_loop(0, OBS // 2, eliminate, h) * mw_ref[0]
    own_b = pl.ds(pl.multiple_of(core * OBS, OBS), OBS)
    aall[own_b, :] = a

    def send_a(slot):
        to = {1: xp, 2: xm, 3: x2}[slot]
        return remote(
            aall.at[own_b, :],
            aall.at[block(2 * slot + core), :],
            as_sem.at[slot - 1],
            ar.at[slot - 1],
            dev(to, y, s, core),
        )

    for slot in (1, 2, 3):
        send_a(slot).start()

    def partner_a(slot):
        ref = aall.at[block(2 * slot + core), :]
        return remote(ref, ref, aps.at[slot], apr.at[slot], dev(x, y, s, other))

    def recv_partner_a(slot):
        ref = aall.at[block(2 * slot + other), :]
        return remote(ref, ref, aps.at[slot], apr.at[slot], dev(x, y, s, other))

    partner_a(0).start()

    z_row = jnp.sum(a * obs_col, axis=0, keepdims=True)
    z_hi, z_lo = split(z_row)
    z_two = jnp.concatenate([z_hi.astype(F32), z_lo.astype(F32), jnp.zeros((14, 128), F32)], axis=0)
    z_two = z_two[:, :OBS].astype(BF16)
    a_hi, a_lo = split(a[:, :OBS])
    for c in range(NCHUNK):
        mine = dall[c, own_b, :]
        res = dot(z_two, mine)
        res = res[0:1] + res[1:2]
        for t in range(5):
            tile = 5 * c + t
            vsend[tile // 10, pl.ds(tile % 10, 1), :] = res[:, 128 * t : 128 * t + 128]
        if c >= 4:
            red = dot(a_hi, mine) + dot(a_lo, mine)
            tail = jnp.sum(mine.astype(F32) * red, axis=0, keepdims=True)
            for t in range(5):
                vsend[c - 4, pl.ds(10 + t, 1), :] = tail[:, 128 * t : 128 * t + 128]
    for k in range(4):
        vsend[k, pl.ds(15, 1), :] = jnp.zeros((1, 128), F32)

    v_to = [(x, other), (xp, core), (xp, other), (xm, core), (xm, other), (x2, core), (x2, other)]

    def send_v(k):
        dx, dc = v_to[k]
        return remote(vsend.at[dx], vall.at[k], vs_sem.at[k], vr.at[k], dev(dx, y, s, dc))

    for k in range(7):
        send_v(k).start()

    prow = iota((ROWS, CHUNK), 0)
    pcol = iota((ROWS, CHUNK), 1)
    pj = prow >> 3
    py = (pj >= 10).astype(jnp.int32) + (pj >= 20).astype(jnp.int32) + (pj >= 30).astype(jnp.int32)
    target = 80 * (prow & 7) + 20 * py + 10 * core + (pj - 10 * py)
    for half in range(2):
        hit = (pcol == target) if half == 0 else ((CHUNK - 1 - pcol) == target)
        picks[half] = jnp.where(hit, 1.0, 0.0).astype(BF16)

    recv_x(1, xp).wait_recv()
    fwd_p(xp).start()
    recv_x(2, 7 - xm).wait_recv()
    fwd_m(xm).start()
    own_lower(1)
    own_upper(1)
    own_lower(2)
    own_upper(2)
    own_lower(3)

    for slot in (1, 2):
        for c in (x, 7 - x):
            recv_x(slot, c).wait_recv()
            partner(slot, c).start()
    for slot in (1, 2, 3):
        send_a(slot).wait_recv()
        partner_a(slot).start()
    for c in (x, 7 - x):
        recv_x(3, c).wait_recv()
        partner(3, c).start()
    for slot in range(4):
        recv_partner_a(slot).wait_recv()

    for b in range(8):
        sel = (iota((128, CHUNK), 1) - OBS * b == iota((128, CHUNK), 0)).astype(F32).astype(BF16)
        hi, lo = split(aall[b * OBS : (b + 1) * OBS, :])
        ahi[b * OBS : (b + 1) * OBS, :] = dot(hi, sel).astype(BF16)
        alo[b * OBS : (b + 1) * OBS, :] = dot(lo, sel).astype(BF16)


    for k in range(7):
        send_v(k).wait_recv()
    vsum = vsend[x]
    for k in range(7):
        vsum = vsum + vall[k]
    row32 = iota((32, 128), 0)
    lane32 = iota((32, 128), 1)
    spread = jnp.zeros((32, 128), F32)
    for rho in range(15):
        if rho < 10:
            start = 160 * (row32 & 7) + 40 * (row32 >> 3) + 20 * core
            width, at, off = 20, 128 * rho, 0
        else:
            start = 80 * (row32 & 7) + 20 * (row32 >> 3) + 10 * core
            width, at, off = 10, 128 * (rho - 10), 20
        idx = lane32 + at
        keep = (idx >= start) & (idx < start + width)
        vals = jnp.where(keep, jnp.broadcast_to(vsum[rho : rho + 1], (32, 128)), 0.0)
        src = iota((128, 128), 0) + at
        place = iota((128, 128), 1) - off
        quot = (src * (3277 if width == 20 else 6554)) >> 16
        q = jnp.where(src - width * quot == place, 1.0, 0.0).astype(BF16)
        hi, lo = split(vals)
        spread = spread + dot(hi, q) + dot(lo, q)
    for yy in range(4):
        extra = jnp.concatenate([spread[8 * yy : 8 * yy + 8], jnp.zeros((8, 128), F32)], axis=0)
        bout[x, yy, 400:416, :] = extra.astype(BF16)

    for slot in range(4):
        recv_partner(slot, x).wait_recv()
        recv_partner(slot, 7 - x).wait_recv()

    for half in range(2):
        chosen = dot_t(picks[half], dall[x if half == 0 else 7 - x]).astype(BF16)
        tt[half] = (dot(chosen, ahi[...]) + dot(chosen, alo[...])).astype(BF16)

    order = [pair(e, x) for e in range(4)]

    def put(q, val):
        for yy in range(4):
            for t in range(5):
                bout[q, yy, 80 * t : 80 * t + 80, :] = val[
                    80 * yy : 80 * yy + 80, 128 * t : 128 * t + 128
                ].astype(BF16)

    rev = jnp.where(iota((128, 128), 0) + iota((128, 128), 1) == 127, 1.0, 0.0).astype(BF16)

    def mirrored(c):
        whole = dall[c]
        parts = []
        for t in range(5):
            parts.append(dot(whole[:, 128 * (4 - t) : 128 * (4 - t) + 128], rev).astype(BF16))
        return jnp.concatenate(parts, axis=1)

    def y_first(q, up, rows):
        near = yp if up else ym
        far2 = (y + 2) % 4
        part = pl.ds(0, rows)
        return remote(
            bout.at[q, far2, part],
            rrel.at[q, part],
            ys1.at[q],
            yr1.at[q],
            dev(x, near, s, core),
        )

    def y_back(q, up, rows):
        far = ym if up else yp
        part = pl.ds(0, rows)
        return remote(
            bout.at[q, far, part],
            rdir.at[q, part],
            ys2.at[q],
            yr2.at[q],
            dev(x, far, s, core),
        )

    def y_sum(q, up, rows):
        near = yp if up else ym
        part = pl.ds(0, rows)
        return remote(
            bout.at[q, near, part],
            rsum.at[q, part],
            ys3.at[q],
            yr3.at[q],
            dev(x, near, s, core),
        )

    def y_parts(e):
        p = order[e]
        return ((7 - p, False, BODY), (p, True, UNIT if e == 0 else BODY))

    def y_send(e):
        for part in y_parts(e):
            y_first(*part).start()
        for part in y_parts(e):
            y_back(*part).start()

    def y_relay(e):
        for part in y_parts(e):
            q, up, rows = part
            near = yp if up else ym
            y_first(*part).wait_recv()
            mine = bout[q, near, 0:rows, :].astype(F32)
            bout[q, near, 0:rows, :] = (mine + rrel[q, 0:rows, :].astype(F32)).astype(BF16)
            y_sum(*part).start()

    def outputs(e):
        p = order[e]
        put(7 - p, dot(tt[0], dall[7 - p]))
        if e < 2:
            y_first(*y_parts(e)[0]).start()
        if e == 0:
            put(p, jnp.where(pcol >= target, dot(tt[0], dall[p]), dot(tt[1], mirrored(7 - p))))
        else:

            @pl.when(p > x)
            def _():
                put(p, dot(tt[0], dall[p]))

            @pl.when(p < x)
            def _():
                put(p, dot(tt[1], mirrored(7 - p)))

        if e < 2:
            y_first(*y_parts(e)[1]).start()
            for part in y_parts(e):
                y_back(*part).start()

    def z_copy(p, d):
        to = (s + d) % NZ
        return remote(zs.at[p, to], zr.at[p, s], zs_sem.at[p, to], zr_sem.at[p, s], dev(x, y, to, core))

    def z_recv(p, d):
        frm = (s + d) % NZ
        return remote(zs.at[p, frm], zr.at[p, frm], zs_sem.at[p, frm], zr_sem.at[p, frm], dev(x, y, frm, core))

    zf[...] = jnp.zeros(zf.shape, F32)

    def y_final(e):
        p = order[e]
        for part in y_parts(e):
            q, up, rows = part
            y_back(*part).wait_recv()
            y_sum(*part).wait_recv()
            total = bout[q, y, 0:rows, :].astype(F32) + rdir[q, 0:rows, :].astype(F32)
            fz[1 - int(up), 0:rows, :] = total + rsum[q, 0:rows, :].astype(F32)
        for k in range(NZ):
            zf[k, 0:50, :] = fz[0, pl.ds(k, 50, stride=8), :]
            zf[k, 50:100, :] = fz[1, pl.ds(k, 50, stride=8), :]
            if e == 0:
                zf[k, 100:101, :] = fz[0, 400 + k : 401 + k, :]
            zs[p, k] = zf[k].astype(BF16)
        for d in range(1, NZ):
            z_copy(p, d).start()

    def z_final(e):
        p = order[e]
        total = zs[p, s].astype(F32)
        for d in range(1, NZ):
            z_recv(p, d).wait_recv()
            total = total + zr[p, (s + d) % NZ].astype(F32)
        of[...] = total
        for half, q in enumerate((p, 7 - p)):
            for t in range(5):
                at = pl.ds(pl.multiple_of(q * CHUNK + 128 * t, 128), 128)
                out_ref[:, at] = of[50 * half + 10 * t : 50 * half + 10 * t + 10, :]
        if e == 0:
            right_ref[...] = of[100:101, 0:20]
            tail_ref[...] = of[100:101, 20:30]

    def relays(e):
        pp = pair(e, xp)
        pm = pair(e, xm)
        need_p = pp != x
        need_m = pm != x
        if e > 1:
            need_p = need_p & (pp != pair(1, x))
            need_m = need_m & (pm != pair(1, x))

        @pl.when(need_p)
        def _():
            recv_x(1, pp).wait_recv()

        fwd_p(pp).start()

        @pl.when(need_m)
        def _():
            recv_x(2, 7 - pm).wait_recv()

        fwd_m(pm).start()

    def line(e, slots):
        p = pair(e, x)
        if e == 1 and 1 in slots:

            @pl.when((p != xp) & (p != pair(1, xp)))
            def _():
                recv_x(1, p).wait_recv()

            @pl.when((p != xm) & (p != pair(1, xm)))
            def _():
                recv_x(2, 7 - p).wait_recv()

        for slot in slots:
            for c, upper in ((p, False), (7 - p, True)):
                if slot == 3 or (slot == 1) == upper:
                    recv_x(slot, c).wait_recv()
                partner(slot, c).start()

    def line_end(e):
        p = pair(e, x)
        for slot in range(4):
            recv_partner(slot, p).wait_recv()
            recv_partner(slot, 7 - p).wait_recv()

    outputs(0)
    relays(1)
    own_upper(3)
    line(1, (1, 2))
    y_relay(0)
    line(1, (3,))
    relays(2)
    line_end(1)
    outputs(1)
    relays(3)
    line(2, (1, 2, 3))
    line_end(2)
    outputs(2)
    y_final(0)
    y_relay(1)
    y_send(2)
    line(3, (1, 2, 3))
    line_end(3)
    outputs(3)
    y_final(1)
    y_relay(2)
    y_send(3)
    z_final(0)
    y_final(2)
    y_relay(3)
    z_final(1)
    y_final(3)
    z_final(2)
    z_final(3)

    for c in range(NCHUNK):
        own_p(c).wait_send()
        own_m(c).wait_send()
    for p in range(4):
        fwd_p(p).wait_send()
        fwd_m(p).wait_send()
        partner_a(p).wait_send()
        for c in range(NCHUNK):
            partner(p, c).wait_send()
    for slot in (1, 2, 3):
        send_a(slot).wait_send()
    for k in range(7):
        send_v(k).wait_send()
    for e in range(4):
        for part in y_parts(e):
            y_first(*part).wait_send()
            y_back(*part).wait_send()
            y_sum(*part).wait_send()
    for p in range(4):
        for d in range(1, NZ):
            z_copy(p, d).wait_send()


def on_device(design, nuisance, observed, arc_of_row, nuis_size, kinds, kind_weight, mission_weight):
    vmem = pl.BlockSpec(memory_space=pltpu.VMEM)
    dma = pltpu.SemaphoreType.DMA
    scratch = [
        pltpu.VMEM((OBS, 128), BF16),
        pltpu.VMEM((1, OBS), F32),
        pltpu.VMEM((1, OBS), jnp.int32),
        pltpu.VMEM((1, OBS), jnp.int32),
        pltpu.SMEM((2,), jnp.int32),
        pltpu.SMEM((8,), F32),
        pltpu.SMEM((1,), F32),
        dma((7,)),
        pltpu.VMEM((NCHUNK, 640, CHUNK), BF16),
        pltpu.VMEM((640, 128), F32),
        pltpu.VMEM((4, 16, 128), F32),
        pltpu.VMEM((7, 16, 128), F32),
        pltpu.VMEM((640, 640), BF16),
        pltpu.VMEM((640, 640), BF16),
        pltpu.VMEM((2, ROWS, 640), BF16),
        pltpu.VMEM((2, ROWS, 640), BF16),
        pltpu.VMEM((NCHUNK, 4, UNIT, 128), BF16),
        pltpu.VMEM((NCHUNK, UNIT, 128), BF16),
        pltpu.VMEM((NCHUNK, UNIT, 128), BF16),
        pltpu.VMEM((NCHUNK, UNIT, 128), BF16),
        pltpu.VMEM((2, UNIT, 128), F32),
        pltpu.VMEM((NZ, ZUNIT, 128), F32),
        pltpu.VMEM((4, NZ, ZUNIT, 128), BF16),
        pltpu.VMEM((4, NZ, ZUNIT, 128), BF16),
        pltpu.VMEM((ZUNIT, 128), F32),
        dma((8,)),
        dma((8,)),
        dma((8,)),
        dma((4,)),
        dma((4,)),
        dma((3, 8)),
        dma((4, 8)),
        dma((4, 8)),
        dma((3,)),
        dma((3,)),
        dma((4,)),
        dma((4,)),
        dma((7,)),
        dma((7,)),
        dma((8,)),
        dma((8,)),
        dma((8,)),
        dma((8,)),
        dma((8,)),
        dma((8,)),
        dma((4, 8)),
        dma((4, 8)),
    ]
    fold, right, tail = pl.pallas_call(
        kernel,
        out_shape=(
            jax.ShapeDtypeStruct((10, WIDTH), F32),
            jax.ShapeDtypeStruct((1, 20), F32),
            jax.ShapeDtypeStruct((1, 10), F32),
        ),
        in_specs=[pl.BlockSpec(memory_space=pl.ANY)] * 8,
        out_specs=(vmem, vmem, vmem),
        scratch_shapes=scratch,
        compiler_params=pltpu.CompilerParams(
            collective_id=0, has_side_effects=True, vmem_limit_bytes=56 * 1024 * 1024
        ),
    )(
        nuis_size,
        kind_weight,
        mission_weight,
        design,
        nuisance,
        observed[None, :],
        arc_of_row[None, :],
        kinds[None, :],
    )
    return (fold, right[0], tail[0])


def solution(mesh):
    rows = P(("mission", "arc"))
    wide = P(("mission", "arc"), None)
    return jax.shard_map(
        on_device,
        mesh=mesh,
        in_specs=(wide, wide, rows, rows, rows, rows, P(), P("mission")),
        out_specs=(wide, rows, rows),
        check_vma=False,
    )
```

```python
import jax
import jax.numpy as jnp
from jax import lax
from jax.experimental import pallas as pl
from jax.experimental.pallas import tpu as pltpu
from jax.sharding import PartitionSpec as P

NX = 4
NY = 4
NZ = 8
OBS = 80
WIDTH = 5120
CHUNK = 640
NCHUNK = 8
ROWS = 320
UNIT = 416
BODY = 400
ZUNIT = 112
F32 = jnp.float32
BF16 = jnp.bfloat16
MESH = pl.DeviceIdType.MESH


def split(v):
    hi = v.astype(BF16)
    lo = (v - hi.astype(F32)).astype(BF16)
    return hi, lo


def iota(shape, dim):
    return lax.broadcasted_iota(jnp.int32, shape, dim)


def dot(a, b):
    return jnp.dot(a, b, preferred_element_type=F32)


def dot_t(a, b):
    return lax.dot_general(a, b, (((1,), (1,)), ((), ())), preferred_element_type=F32)


def kernel(
    ns_in,
    kw_in,
    mw_in,
    design_ref,
    nuis_in,
    obs_in,
    arc_in,
    kind_in,
    out_ref,
    right_ref,
    tail_ref,
    nuis_ref,
    obs_ref,
    arc_ref,
    kind_ref,
    ns_ref,
    kw_ref,
    mw_ref,
    in_sem,
    dall,
    aall,
    vsend,
    vall,
    ahi,
    alo,
    picks,
    tt,
    bout,
    rrel,
    rdir,
    rsum,
    fz,
    zf,
    zs,
    zr,
    of,
    ld_sem,
    xs_p,
    xs_m,
    xf_p,
    xf_m,
    xr,
    ps,
    pr,
    as_sem,
    ar,
    aps,
    apr,
    vs_sem,
    vr,
    ys1,
    ys2,
    ys3,
    yr1,
    yr2,
    yr3,
    zs_sem,
    zr_sem,
):
    mission = lax.axis_index("mission")
    arc = lax.axis_index("arc")
    x = mission // 2
    zl = mission % 2
    zh = arc // 8
    y = (arc // 2) % 4
    core = arc % 2
    s = 4 * zl + zh
    other = 1 - core

    def dev(dx, dy, ds, dc):
        return (2 * dx + ds // 4, 8 * (ds % 4) + 2 * dy + dc)

    xp = (x + 1) % 4
    xm = (x + 3) % 4
    x2 = (x + 2) % 4
    yp = (y + 1) % 4
    ym = (y + 3) % 4

    def block(b):
        return pl.ds(pl.multiple_of(b * OBS, OBS), OBS)

    def load(c):
        return pltpu.make_async_copy(
            design_ref.at[:, pl.ds(c * CHUNK, CHUNK)],
            dall.at[c, block(core), :],
            ld_sem.at[c],
        )

    small_loads = [
        pltpu.make_async_copy(src, dst, in_sem.at[k])
        for k, (src, dst) in enumerate(
            (
                (nuis_in, nuis_ref),
                (obs_in, obs_ref),
                (arc_in, arc_ref),
                (kind_in, kind_ref),
                (ns_in, ns_ref),
                (kw_in, kw_ref),
                (mw_in, mw_ref),
            )
        )
    ]
    for c in range(NCHUNK):
        load(c).start()
    for copy in small_loads:
        copy.start()

    barrier = pltpu.get_barrier_semaphore()
    peers = [dev(xp, y, s, core), dev(xm, y, s, core), dev(x2, y, s, core)]
    peers += [dev(xp, y, s, other), dev(xm, y, s, other), dev(x2, y, s, other)]
    peers += [dev(x, y, s, other), dev(x, yp, s, core), dev(x, ym, s, core)]
    for d in range(1, NZ):
        peers.append(dev(x, y, (s + d) % NZ, core))
    for peer in peers:
        pl.semaphore_signal(barrier, inc=1, device_id=peer, device_id_type=MESH)
    pl.semaphore_wait(barrier, len(peers))

    def remote(src, dst, ssem, rsem, to):
        return pltpu.make_async_remote_copy(
            src_ref=src, dst_ref=dst, send_sem=ssem, recv_sem=rsem, device_id=to, device_id_type=MESH
        )

    def own_p(c):
        return remote(
            dall.at[c, block(core), :],
            dall.at[c, block(2 + core), :],
            xs_p.at[c],
            xr.at[0, c],
            dev(xp, y, s, core),
        )

    def own_m(c):
        return remote(
            dall.at[c, block(core), :],
            dall.at[c, block(4 + core), :],
            xs_m.at[c],
            xr.at[1, c],
            dev(xm, y, s, core),
        )

    def fwd_p(p):
        return remote(
            dall.at[p, block(2 + core), :],
            dall.at[p, block(6 + core), :],
            xf_p.at[p],
            xr.at[2, p],
            dev(xp, y, s, core),
        )

    def fwd_m(p):
        c = 7 - p
        return remote(
            dall.at[c, block(4 + core), :],
            dall.at[c, block(6 + core), :],
            xf_m.at[p],
            xr.at[2, c],
            dev(xm, y, s, core),
        )

    def recv_x(slot, c):
        ref = dall.at[c, block(2 * slot + core), :]
        return remote(ref, ref, xs_p.at[c], xr.at[slot - 1, c], dev(xp, y, s, core))

    def partner(slot, c):
        ref = dall.at[c, block(2 * slot + core), :]
        return remote(ref, ref, ps.at[slot, c], pr.at[slot, c], dev(x, y, s, other))

    def recv_partner(slot, c):
        ref = dall.at[c, block(2 * slot + other), :]
        return remote(ref, ref, ps.at[slot, c], pr.at[slot, c], dev(x, y, s, other))

    def pair(e, mine):
        if e == 0:
            return mine
        return (e - 1) + (e - 1 >= mine).astype(jnp.int32)

    for c in range(NCHUNK):
        load(c).wait()

    own_p(xp).start()
    own_m(7 - xm).start()
    own_p(7 - xp).start()
    own_m(xm).start()
    own_p(x2).start()
    own_m(7 - x2).start()

    for e in range(4):
        p = pair(e, x)
        partner(0, p).start()
        partner(0, 7 - p).start()

    def own_lower(e):
        pp = pair(e, xp)
        pm = pair(e, xm)

        @pl.when(pp != x2)
        def _():
            own_p(pp).start()

        own_m(pm).start()

    def own_upper(e):
        pp = pair(e, xp)
        pm = pair(e, xm)
        own_p(7 - pp).start()

        @pl.when(pm != x2)
        def _():
            own_m(7 - pm).start()

    for copy in small_loads:
        copy.wait()

    lane = iota((OBS, 128), 1)
    sub = iota((OBS, 128), 0)
    eye = lane == sub
    arc_row = jnp.concatenate([arc_ref[...], jnp.full((1, 48), 2, jnp.int32)], axis=1).astype(F32)
    kind_row = jnp.concatenate([kind_ref[...], jnp.zeros((1, 48), jnp.int32)], axis=1)
    obs_row = jnp.concatenate([obs_ref[...], jnp.zeros((1, 48), F32)], axis=1)
    w_row = jnp.zeros((1, 128), F32)
    for k in range(8):
        w_row = jnp.where(kind_row == k, kw_ref[k], w_row)

    def to_col(row):
        return jnp.sum(jnp.where(eye, jnp.broadcast_to(row, (OBS, 128)), 0.0), axis=1, keepdims=True)

    arc_col = to_col(arc_row)
    obs_col = to_col(obs_row)
    size_col = jnp.where(arc_col == 0.0, ns_ref[0], ns_ref[1])
    nuis = jnp.where(lane < size_col, nuis_ref[...].astype(F32), 0.0)
    nuis = jnp.concatenate([nuis, jnp.zeros((48, 128), F32)], axis=0).astype(BF16)
    gram = dot_t(nuis, nuis)[:OBS]
    h = jnp.where(arc_col == arc_row, gram, 0.0) + jnp.where(eye, 1.0 / w_row, 0.0)

    def eliminate(step, h):
        k = 2 * step
        on1 = lane == k
        on2 = lane == k + 1
        at1 = on1[:1]
        at2 = on2[:1]
        is1 = sub == k
        is2 = sub == k + 1
        col1 = jnp.sum(jnp.where(on1, h, 0.0), axis=1, keepdims=True)
        col2 = jnp.sum(jnp.where(on2, h, 0.0), axis=1, keepdims=True)
        row1 = jnp.sum(jnp.where(is1, h, 0.0), axis=0, keepdims=True)
        row2 = jnp.sum(jnp.where(is2, h, 0.0), axis=0, keepdims=True)
        p11 = jnp.sum(jnp.where(at1, row1, 0.0), axis=1, keepdims=True)
        p12 = jnp.sum(jnp.where(at2, row1, 0.0), axis=1, keepdims=True)
        p22 = jnp.sum(jnp.where(at2, row2, 0.0), axis=1, keepdims=True)
        inv = 1.0 / (p11 * p22 - p12 * p12)
        row1 = jnp.where(at1, 1.0, jnp.where(at2, 0.0, row1))
        row2 = jnp.where(at2, 1.0, jnp.where(at1, 0.0, row2))
        new1 = (p22 * inv) * row1 - (p12 * inv) * row2
        new2 = (p11 * inv) * row2 - (p12 * inv) * row1
        rest = jnp.where(on1 | on2, 0.0, h) - col1 * new1 - col2 * new2
        return jnp.where(is1, new1, jnp.where(is2, new2, rest))

    a = lax.fori_loop(0, OBS // 2, eliminate, h) * mw_ref[0]
    own_b = pl.ds(pl.multiple_of(core * OBS, OBS), OBS)
    aall[own_b, :] = a

    def send_a(slot):
        to = {1: xp, 2: xm, 3: x2}[slot]
        return remote(
            aall.at[own_b, :],
            aall.at[block(2 * slot + core), :],
            as_sem.at[slot - 1],
            ar.at[slot - 1],
            dev(to, y, s, core),
        )

    for slot in (1, 2, 3):
        send_a(slot).start()

    def partner_a(slot):
        ref = aall.at[block(2 * slot + core), :]
        return remote(ref, ref, aps.at[slot], apr.at[slot], dev(x, y, s, other))

    def recv_partner_a(slot):
        ref = aall.at[block(2 * slot + other), :]
        return remote(ref, ref, aps.at[slot], apr.at[slot], dev(x, y, s, other))

    partner_a(0).start()

    z_row = jnp.sum(a * obs_col, axis=0, keepdims=True)
    z_hi, z_lo = split(z_row)
    z_two = jnp.concatenate([z_hi.astype(F32), z_lo.astype(F32), jnp.zeros((14, 128), F32)], axis=0)
    z_two = z_two[:, :OBS].astype(BF16)
    a_hi, a_lo = split(a[:, :OBS])
    for c in range(NCHUNK):
        mine = dall[c, own_b, :]
        res = dot(z_two, mine)
        res = res[0:1] + res[1:2]
        for t in range(5):
            tile = 5 * c + t
            vsend[tile // 10, pl.ds(tile % 10, 1), :] = res[:, 128 * t : 128 * t + 128]
        if c >= 4:
            red = dot(a_hi, mine) + dot(a_lo, mine)
            tail = jnp.sum(mine.astype(F32) * red, axis=0, keepdims=True)
            for t in range(5):
                vsend[c - 4, pl.ds(10 + t, 1), :] = tail[:, 128 * t : 128 * t + 128]
    for k in range(4):
        vsend[k, pl.ds(15, 1), :] = jnp.zeros((1, 128), F32)

    v_to = [(x, other), (xp, core), (xp, other), (xm, core), (xm, other), (x2, core), (x2, other)]

    def send_v(k):
        dx, dc = v_to[k]
        return remote(vsend.at[dx], vall.at[k], vs_sem.at[k], vr.at[k], dev(dx, y, s, dc))

    for k in range(7):
        send_v(k).start()

    prow = iota((ROWS, CHUNK), 0)
    pcol = iota((ROWS, CHUNK), 1)
    pj = prow >> 3
    py = (pj >= 10).astype(jnp.int32) + (pj >= 20).astype(jnp.int32) + (pj >= 30).astype(jnp.int32)
    target = 80 * (prow & 7) + 20 * py + 10 * core + (pj - 10 * py)
    for half in range(2):
        hit = (pcol == target) if half == 0 else ((CHUNK - 1 - pcol) == target)
        picks[half] = jnp.where(hit, 1.0, 0.0).astype(BF16)

    recv_x(1, xp).wait_recv()
    fwd_p(xp).start()
    recv_x(2, 7 - xm).wait_recv()
    fwd_m(xm).start()
    own_lower(1)
    own_upper(1)
    own_lower(2)
    own_upper(2)

    for slot in (1, 2):
        for c in (x, 7 - x):
            recv_x(slot, c).wait_recv()
            partner(slot, c).start()
    for slot in (1, 2, 3):
        send_a(slot).wait_recv()
        partner_a(slot).start()
    for c in (x, 7 - x):
        recv_x(3, c).wait_recv()
        partner(3, c).start()
    for slot in range(4):
        recv_partner_a(slot).wait_recv()

    for b in range(8):
        sel = (iota((128, CHUNK), 1) - OBS * b == iota((128, CHUNK), 0)).astype(F32).astype(BF16)
        hi, lo = split(aall[b * OBS : (b + 1) * OBS, :])
        ahi[b * OBS : (b + 1) * OBS, :] = dot(hi, sel).astype(BF16)
        alo[b * OBS : (b + 1) * OBS, :] = dot(lo, sel).astype(BF16)


    for k in range(7):
        send_v(k).wait_recv()
    vsum = vsend[x]
    for k in range(7):
        vsum = vsum + vall[k]
    row32 = iota((32, 128), 0)
    lane32 = iota((32, 128), 1)
    spread = jnp.zeros((32, 128), F32)
    for rho in range(15):
        if rho < 10:
            start = 160 * (row32 & 7) + 40 * (row32 >> 3) + 20 * core
            width, at, off = 20, 128 * rho, 0
        else:
            start = 80 * (row32 & 7) + 20 * (row32 >> 3) + 10 * core
            width, at, off = 10, 128 * (rho - 10), 20
        idx = lane32 + at
        keep = (idx >= start) & (idx < start + width)
        vals = jnp.where(keep, jnp.broadcast_to(vsum[rho : rho + 1], (32, 128)), 0.0)
        src = iota((128, 128), 0) + at
        place = iota((128, 128), 1) - off
        quot = (src * (3277 if width == 20 else 6554)) >> 16
        q = jnp.where(src - width * quot == place, 1.0, 0.0).astype(BF16)
        hi, lo = split(vals)
        spread = spread + dot(hi, q) + dot(lo, q)
    for yy in range(4):
        extra = jnp.concatenate([spread[8 * yy : 8 * yy + 8], jnp.zeros((8, 128), F32)], axis=0)
        bout[x, yy, 400:416, :] = extra.astype(BF16)

    for slot in range(4):
        recv_partner(slot, x).wait_recv()
        recv_partner(slot, 7 - x).wait_recv()

    for half in range(2):
        chosen = dot_t(picks[half], dall[x if half == 0 else 7 - x]).astype(BF16)
        for c0, c1, r0, r1 in ((0, 256, 0, 384), (256, 512, 128, 640), (512, 640, 384, 640)):
            left = chosen[:, r0:r1]
            part = dot(left, ahi[r0:r1, c0:c1]) + dot(left, alo[r0:r1, c0:c1])
            tt[half, :, c0:c1] = part.astype(BF16)

    order = [pair(e, x) for e in range(4)]

    def put(q, val):
        for yy in range(4):
            for t in range(5):
                bout[q, yy, 80 * t : 80 * t + 80, :] = val[
                    80 * yy : 80 * yy + 80, 128 * t : 128 * t + 128
                ].astype(BF16)

    rev = jnp.where(iota((128, 128), 0) + iota((128, 128), 1) == 127, 1.0, 0.0).astype(BF16)

    def mirrored(c):
        whole = dall[c]
        parts = []
        for t in range(5):
            parts.append(dot(whole[:, 128 * (4 - t) : 128 * (4 - t) + 128], rev).astype(BF16))
        return jnp.concatenate(parts, axis=1)

    def y_first(q, up, rows):
        near = yp if up else ym
        far2 = (y + 2) % 4
        part = pl.ds(0, rows)
        return remote(
            bout.at[q, far2, part],
            rrel.at[q, part],
            ys1.at[q],
            yr1.at[q],
            dev(x, near, s, core),
        )

    def y_back(q, up, rows):
        far = ym if up else yp
        part = pl.ds(0, rows)
        return remote(
            bout.at[q, far, part],
            rdir.at[q, part],
            ys2.at[q],
            yr2.at[q],
            dev(x, far, s, core),
        )

    def y_sum(q, up, rows):
        near = yp if up else ym
        part = pl.ds(0, rows)
        return remote(
            bout.at[q, near, part],
            rsum.at[q, part],
            ys3.at[q],
            yr3.at[q],
            dev(x, near, s, core),
        )

    def y_parts(e):
        p = order[e]
        return ((7 - p, False, BODY), (p, True, UNIT if e == 0 else BODY))

    def y_send(e):
        for part in y_parts(e):
            y_first(*part).start()
        for part in y_parts(e):
            y_back(*part).start()

    def y_relay(e):
        for part in y_parts(e):
            q, up, rows = part
            near = yp if up else ym
            y_first(*part).wait_recv()
            mine = bout[q, near, 0:rows, :].astype(F32)
            bout[q, near, 0:rows, :] = (mine + rrel[q, 0:rows, :].astype(F32)).astype(BF16)
            y_sum(*part).start()

    def outputs(e):
        p = order[e]
        put(7 - p, dot(tt[0], dall[7 - p]))
        if e < 2:
            y_first(*y_parts(e)[0]).start()
        if e == 0:
            put(p, jnp.where(pcol >= target, dot(tt[0], dall[p]), dot(tt[1], mirrored(7 - p))))
        else:

            @pl.when(p > x)
            def _():
                put(p, dot(tt[0], dall[p]))

            @pl.when(p < x)
            def _():
                put(p, dot(tt[1], mirrored(7 - p)))

        if e < 2:
            y_first(*y_parts(e)[1]).start()
            for part in y_parts(e):
                y_back(*part).start()

    def z_copy(p, d):
        to = (s + d) % NZ
        return remote(zs.at[p, to], zr.at[p, s], zs_sem.at[p, to], zr_sem.at[p, s], dev(x, y, to, core))

    def z_recv(p, d):
        frm = (s + d) % NZ
        return remote(zs.at[p, frm], zr.at[p, frm], zs_sem.at[p, frm], zr_sem.at[p, frm], dev(x, y, frm, core))

    zf[...] = jnp.zeros(zf.shape, F32)

    def y_final(e):
        p = order[e]
        for part in y_parts(e):
            q, up, rows = part
            y_back(*part).wait_recv()
            y_sum(*part).wait_recv()
            total = bout[q, y, 0:rows, :].astype(F32) + rdir[q, 0:rows, :].astype(F32)
            fz[1 - int(up), 0:rows, :] = total + rsum[q, 0:rows, :].astype(F32)
        for k in range(NZ):
            zf[k, 0:50, :] = fz[0, pl.ds(k, 50, stride=8), :]
            zf[k, 50:100, :] = fz[1, pl.ds(k, 50, stride=8), :]
            if e == 0:
                zf[k, 100:101, :] = fz[0, 400 + k : 401 + k, :]
            zs[p, k] = zf[k].astype(BF16)
        for d in range(1, NZ):
            z_copy(p, d).start()

    def z_final(e):
        p = order[e]
        total = zs[p, s].astype(F32)
        for d in range(1, NZ):
            z_recv(p, d).wait_recv()
            total = total + zr[p, (s + d) % NZ].astype(F32)
        of[...] = total
        for half, q in enumerate((p, 7 - p)):
            for t in range(5):
                at = pl.ds(pl.multiple_of(q * CHUNK + 128 * t, 128), 128)
                out_ref[:, at] = of[50 * half + 10 * t : 50 * half + 10 * t + 10, :]
        if e == 0:
            right_ref[...] = of[100:101, 0:20]
            tail_ref[...] = of[100:101, 20:30]

    def relays(e):
        pp = pair(e, xp)
        pm = pair(e, xm)
        need_p = pp != x
        need_m = pm != x
        if e > 1:
            need_p = need_p & (pp != pair(1, x))
            need_m = need_m & (pm != pair(1, x))

        @pl.when(need_p)
        def _():
            recv_x(1, pp).wait_recv()

        fwd_p(pp).start()

        @pl.when(need_m)
        def _():
            recv_x(2, 7 - pm).wait_recv()

        fwd_m(pm).start()

    def line(e, slots):
        p = pair(e, x)
        if e == 1 and 1 in slots:

            @pl.when((p != xp) & (p != pair(1, xp)))
            def _():
                recv_x(1, p).wait_recv()

            @pl.when((p != xm) & (p != pair(1, xm)))
            def _():
                recv_x(2, 7 - p).wait_recv()

        for slot in slots:
            for c, upper in ((p, False), (7 - p, True)):
                if slot == 3 or (slot == 1) == upper:
                    recv_x(slot, c).wait_recv()
                partner(slot, c).start()

    def line_end(e):
        p = pair(e, x)
        for slot in range(4):
            recv_partner(slot, p).wait_recv()
            recv_partner(slot, 7 - p).wait_recv()

    relays(1)
    own_lower(3)
    own_upper(3)
    outputs(0)
    line(1, (1, 2, 3))
    relays(2)
    y_relay(0)
    line_end(1)
    outputs(1)
    relays(3)
    line(2, (1, 2, 3))
    y_relay(1)
    line_end(2)
    outputs(2)
    y_send(2)
    y_final(0)
    line(3, (1, 2, 3))
    line_end(3)
    outputs(3)
    y_final(1)
    y_relay(2)
    y_send(3)
    z_final(0)
    y_final(2)
    y_relay(3)
    z_final(1)
    y_final(3)
    z_final(2)
    z_final(3)

    for c in range(NCHUNK):
        own_p(c).wait_send()
        own_m(c).wait_send()
    for p in range(4):
        fwd_p(p).wait_send()
        fwd_m(p).wait_send()
        partner_a(p).wait_send()
        for c in range(NCHUNK):
            partner(p, c).wait_send()
    for slot in (1, 2, 3):
        send_a(slot).wait_send()
    for k in range(7):
        send_v(k).wait_send()
    for e in range(4):
        for part in y_parts(e):
            y_first(*part).wait_send()
            y_back(*part).wait_send()
            y_sum(*part).wait_send()
    for p in range(4):
        for d in range(1, NZ):
            z_copy(p, d).wait_send()


def on_device(design, nuisance, observed, arc_of_row, nuis_size, kinds, kind_weight, mission_weight):
    vmem = pl.BlockSpec(memory_space=pltpu.VMEM)
    dma = pltpu.SemaphoreType.DMA
    scratch = [
        pltpu.VMEM((OBS, 128), BF16),
        pltpu.VMEM((1, OBS), F32),
        pltpu.VMEM((1, OBS), jnp.int32),
        pltpu.VMEM((1, OBS), jnp.int32),
        pltpu.SMEM((2,), jnp.int32),
        pltpu.SMEM((8,), F32),
        pltpu.SMEM((1,), F32),
        dma((7,)),
        pltpu.VMEM((NCHUNK, 640, CHUNK), BF16),
        pltpu.VMEM((640, 128), F32),
        pltpu.VMEM((4, 16, 128), F32),
        pltpu.VMEM((7, 16, 128), F32),
        pltpu.VMEM((640, 640), BF16),
        pltpu.VMEM((640, 640), BF16),
        pltpu.VMEM((2, ROWS, 640), BF16),
        pltpu.VMEM((2, ROWS, 640), BF16),
        pltpu.VMEM((NCHUNK, 4, UNIT, 128), BF16),
        pltpu.VMEM((NCHUNK, UNIT, 128), BF16),
        pltpu.VMEM((NCHUNK, UNIT, 128), BF16),
        pltpu.VMEM((NCHUNK, UNIT, 128), BF16),
        pltpu.VMEM((2, UNIT, 128), F32),
        pltpu.VMEM((NZ, ZUNIT, 128), F32),
        pltpu.VMEM((4, NZ, ZUNIT, 128), BF16),
        pltpu.VMEM((4, NZ, ZUNIT, 128), BF16),
        pltpu.VMEM((ZUNIT, 128), F32),
        dma((8,)),
        dma((8,)),
        dma((8,)),
        dma((4,)),
        dma((4,)),
        dma((3, 8)),
        dma((4, 8)),
        dma((4, 8)),
        dma((3,)),
        dma((3,)),
        dma((4,)),
        dma((4,)),
        dma((7,)),
        dma((7,)),
        dma((8,)),
        dma((8,)),
        dma((8,)),
        dma((8,)),
        dma((8,)),
        dma((8,)),
        dma((4, 8)),
        dma((4, 8)),
    ]
    fold, right, tail = pl.pallas_call(
        kernel,
        out_shape=(
            jax.ShapeDtypeStruct((10, WIDTH), F32),
            jax.ShapeDtypeStruct((1, 20), F32),
            jax.ShapeDtypeStruct((1, 10), F32),
        ),
        in_specs=[pl.BlockSpec(memory_space=pl.ANY)] * 8,
        out_specs=(vmem, vmem, vmem),
        scratch_shapes=scratch,
        compiler_params=pltpu.CompilerParams(
            collective_id=0, has_side_effects=True, vmem_limit_bytes=56 * 1024 * 1024
        ),
    )(
        nuis_size,
        kind_weight,
        mission_weight,
        design,
        nuisance,
        observed[None, :],
        arc_of_row[None, :],
        kinds[None, :],
    )
    return (fold, right[0], tail[0])


def solution(mesh):
    rows = P(("mission", "arc"))
    wide = P(("mission", "arc"), None)
    return jax.shard_map(
        on_device,
        mesh=mesh,
        in_specs=(wide, wide, rows, rows, rows, rows, P(), P("mission")),
        out_specs=(wide, rows, rows),
        check_vma=False,
    )
```

```python
import jax
import jax.numpy as jnp
from jax import lax
from jax.experimental import pallas as pl
from jax.experimental.pallas import tpu as pltpu
from jax.sharding import PartitionSpec as P

NX = 4
NY = 4
NZ = 8
OBS = 80
WIDTH = 5120
CHUNK = 640
NCHUNK = 8
ROWS = 320
UNIT = 416
BODY = 400
ZUNIT = 112
F32 = jnp.float32
BF16 = jnp.bfloat16
MESH = pl.DeviceIdType.MESH


def split(v):
    hi = v.astype(BF16)
    lo = (v - hi.astype(F32)).astype(BF16)
    return hi, lo


def iota(shape, dim):
    return lax.broadcasted_iota(jnp.int32, shape, dim)


def dot(a, b):
    return jnp.dot(a, b, preferred_element_type=F32)


def dot_t(a, b):
    return lax.dot_general(a, b, (((1,), (1,)), ((), ())), preferred_element_type=F32)


def kernel(
    ns_in,
    kw_in,
    mw_in,
    design_ref,
    nuis_in,
    obs_in,
    arc_in,
    kind_in,
    out_ref,
    right_ref,
    tail_ref,
    nuis_ref,
    obs_ref,
    arc_ref,
    kind_ref,
    ns_ref,
    kw_ref,
    mw_ref,
    in_sem,
    dall,
    aall,
    vsend,
    vall,
    ahi,
    alo,
    picks,
    tt,
    bout,
    rrel,
    rdir,
    rsum,
    fz,
    zf,
    zs,
    zr,
    of,
    ld_sem,
    xs_p,
    xs_m,
    xf_p,
    xf_m,
    xr,
    ps,
    pr,
    as_sem,
    ar,
    aps,
    apr,
    vs_sem,
    vr,
    ys1,
    ys2,
    ys3,
    yr1,
    yr2,
    yr3,
    zs_sem,
    zr_sem,
):
    mission = lax.axis_index("mission")
    arc = lax.axis_index("arc")
    x = mission // 2
    zl = mission % 2
    zh = arc // 8
    y = (arc // 2) % 4
    core = arc % 2
    s = 4 * zl + zh
    other = 1 - core

    def dev(dx, dy, ds, dc):
        return (2 * dx + ds // 4, 8 * (ds % 4) + 2 * dy + dc)

    xp = (x + 1) % 4
    xm = (x + 3) % 4
    x2 = (x + 2) % 4
    yp = (y + 1) % 4
    ym = (y + 3) % 4

    def block(b):
        return pl.ds(pl.multiple_of(b * OBS, OBS), OBS)

    def load(c):
        return pltpu.make_async_copy(
            design_ref.at[:, pl.ds(c * CHUNK, CHUNK)],
            dall.at[c, block(core), :],
            ld_sem.at[c],
        )

    small_loads = [
        pltpu.make_async_copy(src, dst, in_sem.at[k])
        for k, (src, dst) in enumerate(
            (
                (nuis_in, nuis_ref),
                (obs_in, obs_ref),
                (arc_in, arc_ref),
                (kind_in, kind_ref),
                (ns_in, ns_ref),
                (kw_in, kw_ref),
                (mw_in, mw_ref),
            )
        )
    ]
    for c in range(NCHUNK):
        load(c).start()
    for copy in small_loads:
        copy.start()

    barrier = pltpu.get_barrier_semaphore()
    peers = [dev(xp, y, s, core), dev(xm, y, s, core), dev(x2, y, s, core)]
    peers += [dev(xp, y, s, other), dev(xm, y, s, other), dev(x2, y, s, other)]
    peers += [dev(x, y, s, other), dev(x, yp, s, core), dev(x, ym, s, core)]
    for d in range(1, NZ):
        peers.append(dev(x, y, (s + d) % NZ, core))
    for peer in peers:
        pl.semaphore_signal(barrier, inc=1, device_id=peer, device_id_type=MESH)
    pl.semaphore_wait(barrier, len(peers))

    def remote(src, dst, ssem, rsem, to):
        return pltpu.make_async_remote_copy(
            src_ref=src, dst_ref=dst, send_sem=ssem, recv_sem=rsem, device_id=to, device_id_type=MESH
        )

    def own_p(c):
        return remote(
            dall.at[c, block(core), :],
            dall.at[c, block(2 + core), :],
            xs_p.at[c],
            xr.at[0, c],
            dev(xp, y, s, core),
        )

    def own_m(c):
        return remote(
            dall.at[c, block(core), :],
            dall.at[c, block(4 + core), :],
            xs_m.at[c],
            xr.at[1, c],
            dev(xm, y, s, core),
        )

    def fwd_p(p):
        return remote(
            dall.at[p, block(2 + core), :],
            dall.at[p, block(6 + core), :],
            xf_p.at[p],
            xr.at[2, p],
            dev(xp, y, s, core),
        )

    def fwd_m(p):
        c = 7 - p
        return remote(
            dall.at[c, block(4 + core), :],
            dall.at[c, block(6 + core), :],
            xf_m.at[p],
            xr.at[2, c],
            dev(xm, y, s, core),
        )

    def recv_x(slot, c):
        ref = dall.at[c, block(2 * slot + core), :]
        return remote(ref, ref, xs_p.at[c], xr.at[slot - 1, c], dev(xp, y, s, core))

    def partner(slot, c):
        ref = dall.at[c, block(2 * slot + core), :]
        return remote(ref, ref, ps.at[slot, c], pr.at[slot, c], dev(x, y, s, other))

    def recv_partner(slot, c):
        ref = dall.at[c, block(2 * slot + other), :]
        return remote(ref, ref, ps.at[slot, c], pr.at[slot, c], dev(x, y, s, other))

    def pair(e, mine):
        if e == 0:
            return mine
        return (e - 1) + (e - 1 >= mine).astype(jnp.int32)

    for c in range(NCHUNK):
        load(c).wait()

    own_p(xp).start()
    own_m(7 - xm).start()
    own_p(7 - xp).start()
    own_m(xm).start()
    own_p(x2).start()
    own_m(7 - x2).start()

    for e in range(4):
        p = pair(e, x)
        partner(0, p).start()
        partner(0, 7 - p).start()

    def own_lower(e):
        pp = pair(e, xp)
        pm = pair(e, xm)

        @pl.when(pp != x2)
        def _():
            own_p(pp).start()

        own_m(pm).start()

    def own_upper(e):
        pp = pair(e, xp)
        pm = pair(e, xm)
        own_p(7 - pp).start()

        @pl.when(pm != x2)
        def _():
            own_m(7 - pm).start()

    for copy in small_loads:
        copy.wait()

    lane = iota((OBS, 128), 1)
    sub = iota((OBS, 128), 0)
    eye = lane == sub
    arc_row = jnp.concatenate([arc_ref[...], jnp.full((1, 48), 2, jnp.int32)], axis=1).astype(F32)
    kind_row = jnp.concatenate([kind_ref[...], jnp.zeros((1, 48), jnp.int32)], axis=1)
    obs_row = jnp.concatenate([obs_ref[...], jnp.zeros((1, 48), F32)], axis=1)
    w_row = jnp.zeros((1, 128), F32)
    for k in range(8):
        w_row = jnp.where(kind_row == k, kw_ref[k], w_row)

    def to_col(row):
        return jnp.sum(jnp.where(eye, jnp.broadcast_to(row, (OBS, 128)), 0.0), axis=1, keepdims=True)

    arc_col = to_col(arc_row)
    obs_col = to_col(obs_row)
    size_col = jnp.where(arc_col == 0.0, ns_ref[0], ns_ref[1])
    nuis = jnp.where(lane < size_col, nuis_ref[...].astype(F32), 0.0)
    nuis = jnp.concatenate([nuis, jnp.zeros((48, 128), F32)], axis=0).astype(BF16)
    gram = dot_t(nuis, nuis)[:OBS]
    h = jnp.where(arc_col == arc_row, gram, 0.0) + jnp.where(eye, 1.0 / w_row, 0.0)

    def eliminate(step, h):
        k = 2 * step
        on1 = lane == k
        on2 = lane == k + 1
        at1 = on1[:1]
        at2 = on2[:1]
        is1 = sub == k
        is2 = sub == k + 1
        col1 = jnp.sum(jnp.where(on1, h, 0.0), axis=1, keepdims=True)
        col2 = jnp.sum(jnp.where(on2, h, 0.0), axis=1, keepdims=True)
        row1 = jnp.sum(jnp.where(is1, h, 0.0), axis=0, keepdims=True)
        row2 = jnp.sum(jnp.where(is2, h, 0.0), axis=0, keepdims=True)
        p11 = jnp.sum(jnp.where(at1, row1, 0.0), axis=1, keepdims=True)
        p12 = jnp.sum(jnp.where(at2, row1, 0.0), axis=1, keepdims=True)
        p22 = jnp.sum(jnp.where(at2, row2, 0.0), axis=1, keepdims=True)
        inv = 1.0 / (p11 * p22 - p12 * p12)
        row1 = jnp.where(at1, 1.0, jnp.where(at2, 0.0, row1))
        row2 = jnp.where(at2, 1.0, jnp.where(at1, 0.0, row2))
        new1 = (p22 * inv) * row1 - (p12 * inv) * row2
        new2 = (p11 * inv) * row2 - (p12 * inv) * row1
        rest = jnp.where(on1 | on2, 0.0, h) - col1 * new1 - col2 * new2
        return jnp.where(is1, new1, jnp.where(is2, new2, rest))

    a = lax.fori_loop(0, OBS // 2, eliminate, h) * mw_ref[0]
    own_b = pl.ds(pl.multiple_of(core * OBS, OBS), OBS)
    aall[own_b, :] = a

    def send_a(slot):
        to = {1: xp, 2: xm, 3: x2}[slot]
        return remote(
            aall.at[own_b, :],
            aall.at[block(2 * slot + core), :],
            as_sem.at[slot - 1],
            ar.at[slot - 1],
            dev(to, y, s, core),
        )

    for slot in (1, 2, 3):
        send_a(slot).start()

    def partner_a(slot):
        ref = aall.at[block(2 * slot + core), :]
        return remote(ref, ref, aps.at[slot], apr.at[slot], dev(x, y, s, other))

    def recv_partner_a(slot):
        ref = aall.at[block(2 * slot + other), :]
        return remote(ref, ref, aps.at[slot], apr.at[slot], dev(x, y, s, other))

    partner_a(0).start()

    z_row = jnp.sum(a * obs_col, axis=0, keepdims=True)
    z_hi, z_lo = split(z_row)
    z_two = jnp.concatenate([z_hi.astype(F32), z_lo.astype(F32), jnp.zeros((14, 128), F32)], axis=0)
    z_two = z_two[:, :OBS].astype(BF16)
    a_hi, a_lo = split(a[:, :OBS])
    for c in range(NCHUNK):
        mine = dall[c, own_b, :]
        res = dot(z_two, mine)
        res = res[0:1] + res[1:2]
        for t in range(5):
            tile = 5 * c + t
            vsend[tile // 10, pl.ds(tile % 10, 1), :] = res[:, 128 * t : 128 * t + 128]
        if c >= 4:
            red = dot(a_hi, mine) + dot(a_lo, mine)
            tail = jnp.sum(mine.astype(F32) * red, axis=0, keepdims=True)
            for t in range(5):
                vsend[c - 4, pl.ds(10 + t, 1), :] = tail[:, 128 * t : 128 * t + 128]
    for k in range(4):
        vsend[k, pl.ds(15, 1), :] = jnp.zeros((1, 128), F32)

    v_to = [(x, other), (xp, core), (xp, other), (xm, core), (xm, other), (x2, core), (x2, other)]

    def send_v(k):
        dx, dc = v_to[k]
        return remote(vsend.at[dx], vall.at[k], vs_sem.at[k], vr.at[k], dev(dx, y, s, dc))

    for k in range(7):
        send_v(k).start()

    prow = iota((ROWS, CHUNK), 0)
    pcol = iota((ROWS, CHUNK), 1)
    pj = prow >> 3
    py = (pj >= 10).astype(jnp.int32) + (pj >= 20).astype(jnp.int32) + (pj >= 30).astype(jnp.int32)
    target = 80 * (prow & 7) + 20 * py + 10 * core + (pj - 10 * py)
    for half in range(2):
        hit = (pcol == target) if half == 0 else ((CHUNK - 1 - pcol) == target)
        picks[half] = jnp.where(hit, 1.0, 0.0).astype(BF16)

    recv_x(1, xp).wait_recv()
    fwd_p(xp).start()
    recv_x(2, 7 - xm).wait_recv()
    fwd_m(xm).start()
    own_lower(1)
    own_upper(1)
    own_lower(2)
    own_upper(2)

    for slot in (1, 2):
        for c in (x, 7 - x):
            recv_x(slot, c).wait_recv()
            partner(slot, c).start()
    for slot in (1, 2, 3):
        send_a(slot).wait_recv()
        partner_a(slot).start()
    for c in (x, 7 - x):
        recv_x(3, c).wait_recv()
        partner(3, c).start()
    for slot in range(4):
        recv_partner_a(slot).wait_recv()

    for b in range(8):
        sel = (iota((128, CHUNK), 1) - OBS * b == iota((128, CHUNK), 0)).astype(F32).astype(BF16)
        hi, lo = split(aall[b * OBS : (b + 1) * OBS, :])
        ahi[b * OBS : (b + 1) * OBS, :] = dot(hi, sel).astype(BF16)
        alo[b * OBS : (b + 1) * OBS, :] = dot(lo, sel).astype(BF16)


    for k in range(7):
        send_v(k).wait_recv()
    vsum = vsend[x]
    for k in range(7):
        vsum = vsum + vall[k]
    row32 = iota((32, 128), 0)
    lane32 = iota((32, 128), 1)
    spread = jnp.zeros((32, 128), F32)
    for rho in range(15):
        if rho < 10:
            start = 160 * (row32 & 7) + 40 * (row32 >> 3) + 20 * core
            width, at, off = 20, 128 * rho, 0
        else:
            start = 80 * (row32 & 7) + 20 * (row32 >> 3) + 10 * core
            width, at, off = 10, 128 * (rho - 10), 20
        idx = lane32 + at
        keep = (idx >= start) & (idx < start + width)
        vals = jnp.where(keep, jnp.broadcast_to(vsum[rho : rho + 1], (32, 128)), 0.0)
        src = iota((128, 128), 0) + at
        place = iota((128, 128), 1) - off
        quot = (src * (3277 if width == 20 else 6554)) >> 16
        q = jnp.where(src - width * quot == place, 1.0, 0.0).astype(BF16)
        hi, lo = split(vals)
        spread = spread + dot(hi, q) + dot(lo, q)
    for yy in range(4):
        extra = jnp.concatenate([spread[8 * yy : 8 * yy + 8], jnp.zeros((8, 128), F32)], axis=0)
        bout[x, yy, 400:416, :] = extra.astype(BF16)

    for slot in range(4):
        recv_partner(slot, x).wait_recv()
        recv_partner(slot, 7 - x).wait_recv()

    for half in range(2):
        chosen = dot_t(picks[half], dall[x if half == 0 else 7 - x]).astype(BF16)
        for c0, c1, r0, r1 in ((0, 256, 0, 384), (256, 512, 128, 640), (512, 640, 384, 640)):
            left = chosen[:, r0:r1]
            part = dot(left, ahi[r0:r1, c0:c1]) + dot(left, alo[r0:r1, c0:c1])
            tt[half, :, c0:c1] = part.astype(BF16)

    order = [pair(e, x) for e in range(4)]

    def put(q, val):
        for yy in range(4):
            for t in range(5):
                bout[q, yy, 80 * t : 80 * t + 80, :] = val[
                    80 * yy : 80 * yy + 80, 128 * t : 128 * t + 128
                ].astype(BF16)

    rev = jnp.where(iota((128, 128), 0) + iota((128, 128), 1) == 127, 1.0, 0.0).astype(BF16)

    def mirrored(c):
        whole = dall[c]
        parts = []
        for t in range(5):
            parts.append(dot(whole[:, 128 * (4 - t) : 128 * (4 - t) + 128], rev).astype(BF16))
        return jnp.concatenate(parts, axis=1)

    def y_first(q, up, rows):
        near = yp if up else ym
        far2 = (y + 2) % 4
        part = pl.ds(0, rows)
        return remote(
            bout.at[q, far2, part],
            rrel.at[q, part],
            ys1.at[q],
            yr1.at[q],
            dev(x, near, s, core),
        )

    def y_back(q, up, rows):
        far = ym if up else yp
        part = pl.ds(0, rows)
        return remote(
            bout.at[q, far, part],
            rdir.at[q, part],
            ys2.at[q],
            yr2.at[q],
            dev(x, far, s, core),
        )

    def y_sum(q, up, rows):
        near = yp if up else ym
        part = pl.ds(0, rows)
        return remote(
            bout.at[q, near, part],
            rsum.at[q, part],
            ys3.at[q],
            yr3.at[q],
            dev(x, near, s, core),
        )

    def y_parts(e):
        p = order[e]
        return ((7 - p, False, BODY), (p, True, UNIT if e == 0 else BODY))

    def y_send(e):
        for part in y_parts(e):
            y_first(*part).start()
        for part in y_parts(e):
            y_back(*part).start()

    def y_relay(e):
        for part in y_parts(e):
            q, up, rows = part
            near = yp if up else ym
            y_first(*part).wait_recv()
            mine = bout[q, near, 0:rows, :].astype(F32)
            bout[q, near, 0:rows, :] = (mine + rrel[q, 0:rows, :].astype(F32)).astype(BF16)
            y_sum(*part).start()

    def outputs(e):
        p = order[e]
        put(7 - p, dot(tt[0], dall[7 - p]))
        if e < 2:
            y_first(*y_parts(e)[0]).start()
        if e == 0:
            put(p, jnp.where(pcol >= target, dot(tt[0], dall[p]), dot(tt[1], mirrored(7 - p))))
        else:

            @pl.when(p > x)
            def _():
                put(p, dot(tt[0], dall[p]))

            @pl.when(p < x)
            def _():
                put(p, dot(tt[1], mirrored(7 - p)))

        if e < 2:
            y_first(*y_parts(e)[1]).start()
            for part in y_parts(e):
                y_back(*part).start()

    def z_copy(p, d):
        to = (s + d) % NZ
        return remote(zs.at[p, to], zr.at[p, s], zs_sem.at[p, to], zr_sem.at[p, s], dev(x, y, to, core))

    def z_recv(p, d):
        frm = (s + d) % NZ
        return remote(zs.at[p, frm], zr.at[p, frm], zs_sem.at[p, frm], zr_sem.at[p, frm], dev(x, y, frm, core))

    zf[...] = jnp.zeros(zf.shape, F32)

    def y_final(e):
        p = order[e]
        for part in y_parts(e):
            q, up, rows = part
            y_back(*part).wait_recv()
            y_sum(*part).wait_recv()
            total = bout[q, y, 0:rows, :].astype(F32) + rdir[q, 0:rows, :].astype(F32)
            fz[1 - int(up), 0:rows, :] = total + rsum[q, 0:rows, :].astype(F32)
        for k in range(NZ):
            zf[k, 0:50, :] = fz[0, pl.ds(k, 50, stride=8), :]
            zf[k, 50:100, :] = fz[1, pl.ds(k, 50, stride=8), :]
            if e == 0:
                zf[k, 100:101, :] = fz[0, 400 + k : 401 + k, :]
            zs[p, k] = zf[k].astype(BF16)
        for d in range(1, NZ):
            z_copy(p, d).start()

    def z_final(e):
        p = order[e]
        total = zs[p, s].astype(F32)
        for d in range(1, NZ):
            z_recv(p, d).wait_recv()
            total = total + zr[p, (s + d) % NZ].astype(F32)
        of[...] = total
        for half, q in enumerate((p, 7 - p)):
            for t in range(5):
                at = pl.ds(pl.multiple_of(q * CHUNK + 128 * t, 128), 128)
                out_ref[:, at] = of[50 * half + 10 * t : 50 * half + 10 * t + 10, :]
        if e == 0:
            right_ref[...] = of[100:101, 0:20]
            tail_ref[...] = of[100:101, 20:30]

    def relays(e):
        pp = pair(e, xp)
        pm = pair(e, xm)
        need_p = pp != x
        need_m = pm != x
        if e > 1:
            need_p = need_p & (pp != pair(1, x))
            need_m = need_m & (pm != pair(1, x))

        @pl.when(need_p)
        def _():
            recv_x(1, pp).wait_recv()

        fwd_p(pp).start()

        @pl.when(need_m)
        def _():
            recv_x(2, 7 - pm).wait_recv()

        fwd_m(pm).start()

    def line(e, slots):
        p = pair(e, x)
        if e == 1 and 1 in slots:

            @pl.when((p != xp) & (p != pair(1, xp)))
            def _():
                recv_x(1, p).wait_recv()

            @pl.when((p != xm) & (p != pair(1, xm)))
            def _():
                recv_x(2, 7 - p).wait_recv()

        for slot in slots:
            for c, upper in ((p, False), (7 - p, True)):
                if slot == 3 or (slot == 1) == upper:
                    recv_x(slot, c).wait_recv()
                partner(slot, c).start()

    def line_end(e):
        p = pair(e, x)
        for slot in range(4):
            recv_partner(slot, p).wait_recv()
            recv_partner(slot, 7 - p).wait_recv()

    relays(1)
    own_lower(3)
    own_upper(3)
    outputs(0)
    line(1, (1, 2, 3))
    relays(2)
    y_relay(0)
    line_end(1)
    outputs(1)
    relays(3)
    line(2, (1, 2, 3))
    line(3, (1, 2))
    y_relay(1)
    line_end(2)
    outputs(2)
    y_send(2)
    y_final(0)
    line(3, (3,))
    line_end(3)
    outputs(3)
    y_final(1)
    y_relay(2)
    y_send(3)
    z_final(0)
    y_final(2)
    y_relay(3)
    z_final(1)
    y_final(3)
    z_final(2)
    z_final(3)

    for c in range(NCHUNK):
        own_p(c).wait_send()
        own_m(c).wait_send()
    for p in range(4):
        fwd_p(p).wait_send()
        fwd_m(p).wait_send()
        partner_a(p).wait_send()
        for c in range(NCHUNK):
            partner(p, c).wait_send()
    for slot in (1, 2, 3):
        send_a(slot).wait_send()
    for k in range(7):
        send_v(k).wait_send()
    for e in range(4):
        for part in y_parts(e):
            y_first(*part).wait_send()
            y_back(*part).wait_send()
            y_sum(*part).wait_send()
    for p in range(4):
        for d in range(1, NZ):
            z_copy(p, d).wait_send()


def on_device(design, nuisance, observed, arc_of_row, nuis_size, kinds, kind_weight, mission_weight):
    vmem = pl.BlockSpec(memory_space=pltpu.VMEM)
    dma = pltpu.SemaphoreType.DMA
    scratch = [
        pltpu.VMEM((OBS, 128), BF16),
        pltpu.VMEM((1, OBS), F32),
        pltpu.VMEM((1, OBS), jnp.int32),
        pltpu.VMEM((1, OBS), jnp.int32),
        pltpu.SMEM((2,), jnp.int32),
        pltpu.SMEM((8,), F32),
        pltpu.SMEM((1,), F32),
        dma((7,)),
        pltpu.VMEM((NCHUNK, 640, CHUNK), BF16),
        pltpu.VMEM((640, 128), F32),
        pltpu.VMEM((4, 16, 128), F32),
        pltpu.VMEM((7, 16, 128), F32),
        pltpu.VMEM((640, 640), BF16),
        pltpu.VMEM((640, 640), BF16),
        pltpu.VMEM((2, ROWS, 640), BF16),
        pltpu.VMEM((2, ROWS, 640), BF16),
        pltpu.VMEM((NCHUNK, 4, UNIT, 128), BF16),
        pltpu.VMEM((NCHUNK, UNIT, 128), BF16),
        pltpu.VMEM((NCHUNK, UNIT, 128), BF16),
        pltpu.VMEM((NCHUNK, UNIT, 128), BF16),
        pltpu.VMEM((2, UNIT, 128), F32),
        pltpu.VMEM((NZ, ZUNIT, 128), F32),
        pltpu.VMEM((4, NZ, ZUNIT, 128), BF16),
        pltpu.VMEM((4, NZ, ZUNIT, 128), BF16),
        pltpu.VMEM((ZUNIT, 128), F32),
        dma((8,)),
        dma((8,)),
        dma((8,)),
        dma((4,)),
        dma((4,)),
        dma((3, 8)),
        dma((4, 8)),
        dma((4, 8)),
        dma((3,)),
        dma((3,)),
        dma((4,)),
        dma((4,)),
        dma((7,)),
        dma((7,)),
        dma((8,)),
        dma((8,)),
        dma((8,)),
        dma((8,)),
        dma((8,)),
        dma((8,)),
        dma((4, 8)),
        dma((4, 8)),
    ]
    fold, right, tail = pl.pallas_call(
        kernel,
        out_shape=(
            jax.ShapeDtypeStruct((10, WIDTH), F32),
            jax.ShapeDtypeStruct((1, 20), F32),
            jax.ShapeDtypeStruct((1, 10), F32),
        ),
        in_specs=[pl.BlockSpec(memory_space=pl.ANY)] * 8,
        out_specs=(vmem, vmem, vmem),
        scratch_shapes=scratch,
        compiler_params=pltpu.CompilerParams(
            collective_id=0, has_side_effects=True, vmem_limit_bytes=56 * 1024 * 1024
        ),
    )(
        nuis_size,
        kind_weight,
        mission_weight,
        design,
        nuisance,
        observed[None, :],
        arc_of_row[None, :],
        kinds[None, :],
    )
    return (fold, right[0], tail[0])


def solution(mesh):
    rows = P(("mission", "arc"))
    wide = P(("mission", "arc"), None)
    return jax.shard_map(
        on_device,
        mesh=mesh,
        in_specs=(wide, wide, rows, rows, rows, rows, P(), P("mission")),
        out_specs=(wide, rows, rows),
        check_vma=False,
    )
```
